32 devices in a mesh: seq: 4 (over y, x), fsdp: 8 (over z, core).
Axes of the slice: x: 2, y: 2, z: 4, core: 2. Of those that a mesh axis runs over, the one named last changes fastest.
Arguments:
- images: bfloat16 [24, 512, 1152], P('fsdp', 'seq'), may hold values from -6 to 6
- key_mask: int32 [24, 512], P('fsdp'), may hold values from 0 to 1, as said below
- attn_gain: bfloat16 [1152], P('fsdp'), may hold values from 0.25 to 1.75
- attn_shift: bfloat16 [1152], P('fsdp'), may hold values from -3 to 3
- query_weight: bfloat16 [1152, 1152], P('fsdp'), may hold values from -0.1875 to 0.1875
- key_weight: bfloat16 [1152, 1152], P('fsdp'), may hold values from -0.1875 to 0.1875
- value_weight: bfloat16 [1152, 1152], P('fsdp'), may hold values from -0.1875 to 0.1875
- query_bias: bfloat16 [1152], P('fsdp'), may hold values from -3 to 3
- value_bias: bfloat16 [1152], P('fsdp'), may hold values from -0.1796875 to 0.1796875
- out_weight: bfloat16 [1152, 1152], P('fsdp'), may hold values from -1.5 to 1.5
- out_bias: bfloat16 [1152], P('fsdp'), may hold values from -3 to 3
- mlp_gain: bfloat16 [1152], P('fsdp'), may hold values from 0.25 to 1.75
- mlp_shift: bfloat16 [1152], P('fsdp'), may hold values from -3 to 3
- inner_weight: bfloat16 [1152, 4304], P('fsdp'), may hold values from -0.1875 to 0.1875
- inner_bias: bfloat16 [4304], P('fsdp'), may hold values from -3 to 3
- outer_weight: bfloat16 [4304, 1152], P('fsdp'), may hold values from -0.09375 to 0.09375
- outer_bias: bfloat16 [1152], P('fsdp'), may hold values from -3 to 3
- cotangent: bfloat16 [24, 512, 1152], P('fsdp', 'seq'), may hold values from -6 to 6
Outputs:
- layer_out: float32 [24, 512, 1152], P('fsdp', 'seq')
- images_grad: float32 [24, 512, 1152], P('fsdp', 'seq')
- attn_gain_grad: float32 [1152], P('fsdp')
- attn_shift_grad: float32 [1152], P('fsdp')
- query_weight_grad: float32 [1152, 1152], P('fsdp')
- key_weight_grad: float32 [1152, 1152], P('fsdp')
- value_weight_grad: float32 [1152, 1152], P('fsdp')
- query_bias_grad: float32 [1152], P('fsdp')
- value_bias_grad: float32 [1152], P('fsdp')
- out_weight_grad: float32 [1152, 1152], P('fsdp')
- out_bias_grad: float32 [1152], P('fsdp')
- mlp_gain_grad: float32 [1152], P('fsdp')
- mlp_shift_grad: float32 [1152], P('fsdp')
- inner_weight_grad: float32 [1152, 4304], P('fsdp')
- inner_bias_grad: float32 [4304], P('fsdp')
- outer_weight_grad: float32 [4304, 1152], P('fsdp')
- outer_bias_grad: float32 [1152], P('fsdp')
The draws below stay inside these ranges and needn't reach their ends.
Inputs may be any that keep to these rules, and one draw needn't show every extreme that they name: `key_mask`: each image's row is 1 on its first positions and 0 after them; at least 128 positions are 1.
All inputs are finite; a program needn't handle non-finite values.
Results may differ from the reference program's by a relative error of at most 0.013.
The reference program's roundings to bfloat16 on the way count: a program that leaves them out, or rounds other values in their place, can miss the bound.
Values may be sent and summed in bfloat16 or wider, within the bound.
A program may use at most 256 MiB of HBM per device.

```python
import jax
import jax.numpy as jnp
from jax import lax

D = 1152
FF = 4304
H = 16
HD = 72
LEN = 512
IMG_DEV = 3
IMAGES = 24
N_FSDP = 8


def draw_key_mask(key, part):
    counts = jax.random.randint(jax.random.fold_in(key, 11), (IMAGES,), LEN // 4, LEN + 1)
    counts = counts.at[0].set(LEN // 4).at[IMAGES - 1].set(LEN)
    positions = jnp.arange(LEN, dtype=jnp.int32)
    return (positions[None, :] < counts[:, None]).astype(jnp.int32)


def spiked(drawn, own_key, source, target, parts, factor):
    def block_of(dim):
        return (jnp.arange(drawn.shape[dim]) // (drawn.shape[dim] // parts)).reshape((-1,) + (1,) * (drawn.ndim - 1 - dim))

    first = jax.random.permutation(own_key, parts)[block_of(target)]
    second = (block_of(target) + parts // 2) % parts
    return jnp.where((block_of(source) == first) | (block_of(source) == second), factor * drawn, drawn)


def shard_levels(key, extent, split, least, high):
    loudness = 1.0
    for position, blocks in split:
        steps = jax.random.uniform(jax.random.fold_in(jax.random.fold_in(key, 6), position), (blocks,), jnp.float32, least / len(split), high / len(split))
        loudness = loudness * jnp.repeat(jnp.exp(steps), extent[position] // blocks).reshape((-1,) + (1,) * (len(extent) - 1 - position))
    return loudness


def normal_values(own_key, shape, deviation, limit, split=(), kind=jnp.bfloat16):
    values = jax.random.normal(own_key, shape, jnp.float32) * deviation
    if len(split) > 0:
        values = shard_levels(own_key, shape, split, -0.22, 0.18) * values
    return jnp.clip(values, min=-limit, max=limit).astype(kind)


def bell_draw_with(own_key, extent, scale, bound, cuts, heavy, held_as=jnp.bfloat16):
    values = scale * jax.random.normal(own_key, extent, jnp.float32)
    if cuts:
        values = values * shard_levels(own_key, extent, cuts, -0.22, 0.18)
    return jnp.clip(spiked(values, jax.random.fold_in(own_key, 3), *heavy), -bound, bound).astype(held_as)


def setup_inputs(seed: int = 0) -> dict:
    key_of = jax.random.split(jax.random.key(seed), 19)
    return {
        "images": normal_values(key_of[0], (IMAGES, LEN, D), 1.0, 6.0, ((0, 8), (1, 4))),
        "key_mask": draw_key_mask(jax.random.fold_in(key_of[18], 71), 0),
        "attn_gain": jnp.clip(1.0 + 0.15 * jax.random.normal(key_of[2], (D,), jnp.float32), 0.25, 1.75).astype(jnp.bfloat16),
        "attn_shift": normal_values(key_of[3], (D,), 0.5, 3.0, ((0, 8),)),
        "query_weight": normal_values(key_of[4], (D, D), D ** -0.5, 0.1875, ((0, 8),)),
        "key_weight": normal_values(key_of[5], (D, D), D ** -0.5, 0.1875, ((0, 8),)),
        "value_weight": normal_values(key_of[6], (D, D), D ** -0.5, 0.1875, ((0, 8),)),
        "query_bias": normal_values(key_of[7], (D,), 0.5, 3.0, ((0, 8),)),
        "value_bias": normal_values(key_of[8], (D,), 0.03, 0.1796875, ((0, 8),)),
        "out_weight": normal_values(key_of[9], (D, D), (max(D * 8 // LEN, 1)) ** -0.5, 1.5, ((0, 8),)),
        "out_bias": normal_values(key_of[10], (D,), 0.5, 3.0, ((0, 8),)),
        "mlp_gain": jnp.clip(1.0 + 0.15 * jax.random.normal(key_of[11], (D,), jnp.float32), 0.25, 1.75).astype(jnp.bfloat16),
        "mlp_shift": normal_values(key_of[12], (D,), 0.5, 3.0, ((0, 8),)),
        "inner_weight": normal_values(key_of[13], (D, FF), D ** -0.5, 0.1875, ((0, 8),)),
        "inner_bias": normal_values(key_of[14], (FF,), 0.5, 3.0, ((0, 8),)),
        "outer_weight": normal_values(key_of[15], (FF, D), FF ** -0.5, 0.09375, ((0, 8),)),
        "outer_bias": normal_values(key_of[16], (D,), 0.5, 3.0, ((0, 8),)),
        "cotangent": bell_draw_with(key_of[17], (IMAGES, LEN, D), 1.0, 6.0, ((0, 8), (1, 4)), (0, 2, 8, 2.0)),
    }


EPSILON = 1e-06
MASKED = -1e+30

def widen(values):
    return lax.optimization_barrier(values).astype(jnp.float32)

def product(left, right):
    return jnp.dot(left, right, preferred_element_type=jnp.float32)

def product_rows(left, right):
    return jnp.dot(left.T, right, preferred_element_type=jnp.float32)

def product_back(left, right):
    return jnp.dot(left, right.T, preferred_element_type=jnp.float32)

def gelu_tanh(values):
    return jax.nn.gelu(values, approximate=True)

def normalize(values):
    center = values - lax.optimization_barrier(jnp.mean(values, axis=-1, keepdims=True))
    factor = lax.rsqrt(lax.optimization_barrier(jnp.mean(center * center, axis=-1, keepdims=True)) + EPSILON)
    return (center * factor, factor)

def norm_back(grad_normed, normed, factor):
    first = lax.optimization_barrier(jnp.mean(grad_normed, axis=-1, keepdims=True))
    second = lax.optimization_barrier(jnp.mean(grad_normed * normed, axis=-1, keepdims=True))
    return factor * (grad_normed - first - normed * second)

def image_forward(items):
    query, keys, values, valid = items
    scale = HD ** (-0.5)
    block = min(512, LEN)
    key_wide = widen(keys)
    value_wide = widen(values)
    blocks = query.reshape(LEN // block, block, H, HD)

    def visit(query_block):
        scores = jnp.einsum('qhd,khd->hqk', widen(query_block), key_wide) * scale
        scores = jnp.where(valid[None, None, :], scores, MASKED)
        highest = lax.optimization_barrier(jnp.max(scores, axis=-1, keepdims=True))
        logsum = highest + jnp.log(lax.optimization_barrier(jnp.sum(jnp.exp(scores - highest), axis=-1, keepdims=True)))
        attention = jnp.exp(scores - logsum).astype(jnp.bfloat16)
        attended = jnp.einsum('hqk,khd->qhd', widen(attention), value_wide).astype(jnp.bfloat16)
        return (attended, logsum[..., 0])
    attended, logsum = lax.map(visit, blocks)
    return (attended.reshape(LEN, H, HD), logsum)

def image_backward(items):
    query, keys, values, attended, grad_out, logsum, valid = items
    scale = HD ** (-0.5)
    block = min(512, LEN)
    count_blocks = LEN // block
    key_wide = widen(keys)
    value_wide = widen(values)
    blocks = (query.reshape(count_blocks, block, H, HD), attended.reshape(count_blocks, block, H, HD), grad_out.reshape(count_blocks, block, H, HD), logsum)
    zeros = jnp.zeros((LEN, H, HD), jnp.float32)

    def visit(carry, piece):
        query_block, out_block, grad_block, logsum_block = piece
        grad_keys, grad_values = carry
        query_wide = widen(query_block)
        grad_wide = widen(grad_block)
        scores = jnp.einsum('qhd,khd->hqk', query_wide, key_wide) * scale
        scores = jnp.where(valid[None, None, :], scores, MASKED)
        chance = jnp.exp(scores - logsum_block[:, :, None])
        chance_low = chance.astype(jnp.bfloat16)
        grad_values = grad_values + jnp.einsum('hqk,qhd->khd', widen(chance_low), grad_wide)
        grad_chance = jnp.einsum('qhd,khd->hqk', grad_wide, value_wide)
        delta = lax.optimization_barrier(jnp.sum(grad_wide * widen(out_block), axis=-1)).T
        grad_scores = (chance * (grad_chance - delta[:, :, None]) * scale).astype(jnp.bfloat16)
        grad_scores_wide = widen(grad_scores)
        grad_query = jnp.einsum('hqk,khd->qhd', grad_scores_wide, key_wide).astype(jnp.bfloat16)
        grad_keys = grad_keys + jnp.einsum('hqk,qhd->khd', grad_scores_wide, query_wide)
        return ((grad_keys, grad_values), grad_query)
    (grad_keys, grad_values), grad_query = lax.scan(visit, (zeros, zeros), blocks)
    return (grad_query.reshape(LEN, H, HD), grad_keys.astype(jnp.bfloat16), grad_values.astype(jnp.bfloat16))

def group_pass(params, group_images, group_mask, group_cot):
    gain_attn, shift_attn, w_query, w_key, w_value, b_query, b_value, w_out, b_out, gain_mlp, shift_mlp, w_inner, b_inner, w_outer, b_outer = params
    rows = IMG_DEV * LEN
    flat = group_images.reshape(rows, D).astype(jnp.float32)
    normed_one, factor_one = normalize(flat)
    hidden_one = (normed_one * gain_attn.astype(jnp.float32) + shift_attn.astype(jnp.float32)).astype(jnp.bfloat16)
    query = (product(hidden_one, w_query) + b_query.astype(jnp.float32)).astype(jnp.bfloat16)
    keys = product(hidden_one, w_key).astype(jnp.bfloat16)
    values = (product(hidden_one, w_value) + b_value.astype(jnp.float32)).astype(jnp.bfloat16)
    shape_heads = (IMG_DEV, LEN, H, HD)
    query_heads = query.reshape(shape_heads)
    key_heads = keys.reshape(shape_heads)
    value_heads = values.reshape(shape_heads)
    valid = group_mask > 0
    attended, logsum = lax.map(image_forward, (query_heads, key_heads, value_heads, valid))
    attended_flat = attended.reshape(rows, D)
    second = flat + product(attended_flat, w_out) + b_out.astype(jnp.float32)
    normed_two, factor_two = normalize(second)
    hidden_two = (normed_two * gain_mlp.astype(jnp.float32) + shift_mlp.astype(jnp.float32)).astype(jnp.bfloat16)
    inner = product(hidden_two, w_inner) + b_inner.astype(jnp.float32)
    active = gelu_tanh(inner).astype(jnp.bfloat16)
    layer_out = second + product(active, w_outer) + b_outer.astype(jnp.float32)
    upstream = group_cot.reshape(rows, D)
    grad_active = product_back(upstream, w_outer)
    grad_inner = jax.vjp(gelu_tanh, inner)[1](grad_active)[0]
    grad_inner_low = grad_inner.astype(jnp.bfloat16)
    grad_hidden_two = product_back(grad_inner_low, w_inner)
    grad_second = upstream.astype(jnp.float32) + norm_back(grad_hidden_two * gain_mlp.astype(jnp.float32), normed_two, factor_two)
    grad_second_low = grad_second.astype(jnp.bfloat16)
    grad_attended = product_back(grad_second_low, w_out).astype(jnp.bfloat16)
    grad_query, grad_keys, grad_values = lax.map(image_backward, (query_heads, key_heads, value_heads, attended, grad_attended.reshape(shape_heads), logsum, valid))
    grad_query = grad_query.reshape(rows, D)
    grad_keys = grad_keys.reshape(rows, D)
    grad_values = grad_values.reshape(rows, D)
    grad_hidden_one = product_back(grad_query, w_query) + product_back(grad_keys, w_key) + product_back(grad_values, w_value)
    images_grad = grad_second + norm_back(grad_hidden_one * gain_attn.astype(jnp.float32), normed_one, factor_one)
    totals = (lax.optimization_barrier(jnp.sum(grad_hidden_one * normed_one, axis=0)), lax.optimization_barrier(jnp.sum(grad_hidden_one, axis=0)), product_rows(hidden_one, grad_query), product_rows(hidden_one, grad_keys), product_rows(hidden_one, grad_values), lax.optimization_barrier(jnp.sum(widen(grad_query), axis=0)), lax.optimization_barrier(jnp.sum(widen(grad_values), axis=0)), product_rows(attended_flat, grad_second_low), lax.optimization_barrier(jnp.sum(grad_second, axis=0)), lax.optimization_barrier(jnp.sum(grad_hidden_two * normed_two, axis=0)), lax.optimization_barrier(jnp.sum(grad_hidden_two, axis=0)), product_rows(hidden_two, grad_inner_low), lax.optimization_barrier(jnp.sum(grad_inner, axis=0)), product_rows(active, upstream), lax.optimization_barrier(jnp.sum(widen(upstream), axis=0)))
    return (layer_out.reshape(IMG_DEV, LEN, D), images_grad.reshape(IMG_DEV, LEN, D), totals)

def reference(images, key_mask, attn_gain, attn_shift, query_weight, key_weight, value_weight, query_bias, value_bias, out_weight, out_bias, mlp_gain, mlp_shift, inner_weight, inner_bias, outer_weight, outer_bias, cotangent):
    params = (attn_gain, attn_shift, query_weight, key_weight, value_weight, query_bias, value_bias, out_weight, out_bias, mlp_gain, mlp_shift, inner_weight, inner_bias, outer_weight, outer_bias)
    start = jax.tree.map(lambda item: jnp.zeros(item.shape, jnp.float32), params)

    def visit(carry, items):
        group_images, group_mask, group_cot = items
        layer_out, images_grad, totals = group_pass(params, group_images, group_mask, group_cot)
        carry = jax.tree.map(lambda left, right: left + right, carry, totals)
        return (carry, (layer_out, images_grad))
    xs = (images.reshape(N_FSDP, IMG_DEV, LEN, D), key_mask.reshape(N_FSDP, IMG_DEV, LEN), cotangent.reshape(N_FSDP, IMG_DEV, LEN, D))
    grads, (layer_out, images_grad) = lax.scan(visit, start, xs)
    layer_out = layer_out.reshape(IMAGES, LEN, D)
    images_grad = images_grad.reshape(IMAGES, LEN, D)
    return (layer_out, images_grad, grads[0], grads[1], grads[2], grads[3], grads[4], grads[5], grads[6], grads[7], grads[8], grads[9], grads[10], grads[11], grads[12], grads[13], grads[14])
```

```python
import functools

import jax
import jax.numpy as jnp
from jax import lax
from jax.experimental import pallas as pl
from jax.experimental.pallas import tpu as pltpu
from jax.sharding import PartitionSpec as P

HD = 72
EPSILON = 1e-06
MASKED = -1e30
MESH = pl.DeviceIdType.MESH
VMEM_LIMIT = 64_000_000


def flip(index, bit):
    on = lax.rem(lax.div(index, 1 << bit), 2)
    return index + (1 - 2 * on) * (1 << bit)


def flip_mask(index, mask):
    bit = 0
    while mask >> bit:
        if (mask >> bit) & 1:
            index = flip(index, bit)
        bit += 1
    return index


def halving(bits, parts):
    plan = []
    for j in range(parts):
        held, steps, slot = [0], [], 0
        for k in range(bits):
            bit = (j + k) % bits
            steps.append((bit, tuple(held), slot))
            slot += len(held)
            held = held + [m ^ (1 << bit) for m in held]
        plan.append(steps)
    return plan


def copy_to(src, dst, send, recv, seq, fsdp):
    return pltpu.make_async_remote_copy(
        src_ref=src,
        dst_ref=dst,
        send_sem=send,
        recv_sem=recv,
        device_id={"seq": seq, "fsdp": fsdp},
        device_id_type=MESH,
    )


def greet(s, f, n_seq, n_fsdp):
    core, zed = lax.rem(f, 2), lax.div(f, 2)
    n_z = n_fsdp // 2
    barrier = pltpu.get_barrier_semaphore()
    peers = [(s, f + 1 - 2 * core)]
    peers += [(s, lax.rem(zed + d, n_z) * 2 + core) for d in range(1, n_z)]
    bit = 0
    while (1 << bit) < n_seq:
        peers.append((flip(s, bit), f))
        bit += 1
    for seq, fsdp in peers:
        pl.semaphore_signal(
            barrier, inc=1, device_id={"seq": seq, "fsdp": fsdp}, device_id_type=MESH
        )
    pl.semaphore_wait(barrier, len(peers))


def gather_kernel(n_seq, n_fsdp, packs, parts, *refs):
    own = refs[:packs]
    vec = refs[packs]
    full = refs[packs + 1 : 2 * packs + 1]
    vec_full = refs[2 * packs + 1]
    z_send, z_recv, p_send, p_recv, c_send, c_recv, v_send, v_recv, local = refs[2 * packs + 2 :]
    s, f = lax.axis_index("seq"), lax.axis_index("fsdp")
    core, zed = lax.rem(f, 2), lax.div(f, 2)
    n_z = n_fsdp // 2
    bits = n_seq.bit_length() - 1
    plan = halving(bits, parts)
    other = f + 1 - 2 * core
    from_f = [lax.rem(zed - d + n_z, n_z) * 2 + core for d in range(n_z)]
    to_f = [lax.rem(zed + d, n_z) * 2 + core for d in range(n_z)]
    greet(s, f, n_seq, n_fsdp)

    def z_copy(p, d):
        return copy_to(
            own[p].at[s], full[p].at[s, f], z_send.at[p, d], z_recv.at[p, d], s, to_f[d]
        )

    def z_arrival(p, d):
        return copy_to(
            own[p].at[s], full[p].at[s, from_f[d]], z_send.at[p, d], z_recv.at[p, d], s, to_f[d]
        )

    def plane_copies(p, d, k, arriving):
        out = []
        for j in range(parts):
            bit, held, slot = plan[j][k]
            for i, mask in enumerate(held):
                place = full[p].at[flip_mask(s, mask), from_f[d], j]
                arrive = full[p].at[flip_mask(s, mask ^ (1 << bit)), from_f[d], j]
                sems = p_send.at[p, d, j, slot + i], p_recv.at[p, d, j, slot + i]
                target = arrive if arriving else place
                out.append(copy_to(place, target, *sems, flip(s, bit), f))
        return out

    def core_copy(p, d):
        return copy_to(
            full[p].at[:, from_f[d]],
            full[p].at[:, from_f[d]],
            c_send.at[p, d],
            c_recv.at[p, d],
            s,
            other,
        )

    def core_first(p):
        return copy_to(own[p], full[p].at[:, f], c_send.at[p, 0], c_recv.at[p, 0], s, other)

    def core_arrival(p, d):
        place = full[p].at[:, from_f[d] + 1 - 2 * core]
        return copy_to(place, place, c_send.at[p, d], c_recv.at[p, d], s, other)

    sent = []

    def start(copy):
        copy.start()
        sent.append(copy)

    vec_targets = [to_f[d] for d in range(1, n_z)] + [other]
    for i, target in enumerate(vec_targets):
        start(copy_to(vec, vec_full.at[f], v_send.at[i], v_recv.at[i], s, target))
    for p in range(packs):
        for d in range(1, n_z):
            start(z_copy(p, d))
    keep = [pltpu.make_async_copy(own[p], full[p].at[:, f], local.at[p]) for p in range(packs)]
    keep.append(pltpu.make_async_copy(vec, vec_full.at[f], local.at[packs]))
    for copy in keep:
        copy.start()
    for p in range(packs):
        start(core_first(p))
    for d in range(1, n_z):
        copy_to(vec, vec_full.at[from_f[d]], v_send.at[d - 1], v_recv.at[d - 1], s, to_f[d]).wait_recv()
        start(
            copy_to(
                vec_full.at[from_f[d]],
                vec_full.at[from_f[d]],
                v_send.at[n_z - 1 + d],
                v_recv.at[n_z - 1 + d],
                s,
                other,
            )
        )

    def finish(p, d):
        for arrival in plane_copies(p, d, bits - 1, True):
            arrival.wait_recv()
        start(core_copy(p, d))

    for p in range(packs + 1):
        for d in range(1, n_z):
            if p < packs:
                z_arrival(p, d).wait_recv()
                for copy in plane_copies(p, d, 0, False):
                    start(copy)
            if p > 0:
                finish(p - 1, d)
        if p < packs:
            for k in range(1, bits):
                for d in range(1, n_z):
                    for arrival in plane_copies(p, d, k - 1, True):
                        arrival.wait_recv()
                    for copy in plane_copies(p, d, k, False):
                        start(copy)
    for copy in keep:
        copy.wait()
    for p in range(packs):
        for d in range(n_z):
            core_arrival(p, d).wait_recv()
    for d in range(n_z):
        place = vec_full.at[from_f[d] + 1 - 2 * core]
        sem = n_z - 1 + d
        copy_to(place, place, v_send.at[sem], v_recv.at[sem], s, other).wait_recv()
    for copy in sent:
        copy.wait_send()


def gather_all(n_seq, n_fsdp, blocks, vec):
    packs, parts = len(blocks), blocks[0].shape[1]
    n_z = n_fsdp // 2
    dma = pltpu.SemaphoreType.DMA
    out = [
        jax.ShapeDtypeStruct((b.shape[0], n_fsdp) + b.shape[1:], b.dtype) for b in blocks
    ] + [jax.ShapeDtypeStruct((n_fsdp,) + vec.shape, vec.dtype)]
    return pl.pallas_call(
        functools.partial(gather_kernel, n_seq, n_fsdp, packs, parts),
        out_shape=out,
        in_specs=[pl.BlockSpec(memory_space=pltpu.VMEM)] * (packs + 1),
        out_specs=[pl.BlockSpec(memory_space=pl.ANY)] * (packs + 1),
        scratch_shapes=[
            dma((packs, n_z)),
            dma((packs, n_z)),
            dma((packs, n_z, parts, n_seq - 1)),
            dma((packs, n_z, parts, n_seq - 1)),
            dma((packs, n_z)),
            dma((packs, n_z)),
            dma((2 * n_z - 1,)),
            dma((2 * n_z - 1,)),
            dma((packs + 1,)),
        ],
        compiler_params=pltpu.CompilerParams(
            collective_id=0, has_side_effects=True, vmem_limit_bytes=VMEM_LIMIT
        ),
        name="gather_weights",
    )(*blocks, vec)


def add_into(target, term, rows):
    target[...] = (target[...].astype(jnp.float32) + term[...].astype(jnp.float32)).astype(
        target.dtype
    )


def reduce_kernel(n_seq, n_fsdp, packs, parts, *refs):
    share = n_seq // 4
    n_grads = 4 * packs
    grads = refs[:n_grads]
    vec = refs[n_grads]
    out = refs[n_grads + 1 : n_grads + 1 + packs]
    vec_out = refs[n_grads + 1 + packs]
    (
        held,
        part_in,
        plane_in,
        z_in,
        total,
        v_core,
        v_plane,
        v_z,
        v_work,
        l_sem,
        c_send,
        c_recv,
        p_send,
        p_recv,
        z_send,
        z_recv,
        g_send,
        g_recv,
        v_send,
        v_recv,
        o_sem,
    ) = refs[n_grads + 2 + packs :]
    s, f = lax.axis_index("seq"), lax.axis_index("fsdp")
    core, zed = lax.rem(f, 2), lax.div(f, 2)
    n_z = n_fsdp // 2
    bits = n_seq.bit_length() - 1
    plan = halving(bits, parts)
    other = f + 1 - 2 * core
    to_f = [lax.rem(zed + d, n_z) * 2 + core for d in range(n_z)]
    greet(s, f, n_seq, n_fsdp)
    sent = []

    def start(copy):
        copy.start()
        sent.append(copy)

    def target_z(t):
        return lax.rem(zed + t + 1, n_z)

    def load(p, t):
        out = []
        for q in range(n_seq):
            src = grads[4 * p + q // share]
            out.append(
                pltpu.make_async_copy(
                    src.at[2 * target_z(t) + core, q % share],
                    held.at[p, t, q],
                    l_sem.at[p, t, q],
                )
            )
        return out

    def to_partner(p, t):
        out = []
        for q in range(n_seq):
            src = grads[4 * p + q // share]
            out.append(
                copy_to(
                    src.at[2 * target_z(t) + 1 - core, q % share],
                    part_in.at[p, t, q],
                    c_send.at[p, t, q],
                    c_recv.at[p, t, q],
                    s,
                    other,
                )
            )
        return out

    def plane(p, t, k):
        out = []
        for j in range(parts):
            bit, masks, slot = plan[j][k]
            for i, mask in enumerate(masks):
                out.append(
                    (
                        copy_to(
                            held.at[p, t, flip_mask(s, mask ^ (1 << bit)), j],
                            plane_in.at[p, t, j, slot + i],
                            p_send.at[p, t, j, slot + i],
                            p_recv.at[p, t, j, slot + i],
                            flip(s, bit),
                            f,
                        ),
                        held.at[p, t, flip_mask(s, mask), j],
                        plane_in.at[p, t, j, slot + i],
                    )
                )
        return out

    def z_copy(p, t):
        return copy_to(
            held.at[p, t, s],
            z_in.at[p, t],
            z_send.at[p, t],
            z_recv.at[p, t],
            s,
            2 * target_z(t) + core,
        )

    def spread(p, k, arriving):
        out = []
        for j in range(parts):
            bit, masks, slot = plan[j][k]
            for i, mask in enumerate(masks):
                place = total.at[p, flip_mask(s, mask), j]
                arrive = total.at[p, flip_mask(s, mask ^ (1 << bit)), j]
                sems = g_send.at[p, j, slot + i], g_recv.at[p, j, slot + i]
                target = arrive if arriving else place
                out.append(copy_to(place, target, *sems, flip(s, bit), f))
        return out

    chunks = [(p, t) for p in range(packs) for t in range(n_z)]
    v_part = copy_to(
        vec.at[:, 1 - core], v_core, v_send.at[0], v_recv.at[0], s, other
    )
    start(v_part)
    for p, t in chunks:
        for copy in to_partner(p, t):
            start(copy)
        for copy in load(p, t):
            copy.start()

    def stage_core(p, t):
        for copy, arrival in zip(load(p, t), to_partner(p, t)):
            copy.wait()
            arrival.wait_recv()
        for q in range(n_seq):
            add_into(held.at[p, t, q], part_in.at[p, t, q], None)
        for copy, _, _ in plane(p, t, bits - 1):
            start(copy)

    def stage_plane(p, t, k):
        for copy, mine, came in plane(p, t, k):
            copy.wait_recv()
            add_into(mine, came, None)
        if k > 0:
            for copy, _, _ in plane(p, t, k - 1):
                start(copy)
        elif t < n_z - 1:
            start(z_copy(p, t))

    def stage_total(p):
        for t in range(n_z - 1):
            z_copy(p, t).wait_recv()
        for j in range(parts):
            value = held[p, n_z - 1, s, j].astype(jnp.float32)
            for t in range(n_z - 1):
                value = value + z_in[p, t, j].astype(jnp.float32)
            total[p, s, j] = value.astype(total.dtype)
        for copy in spread(p, 0, False):
            start(copy)

    def stage_spread(p, k):
        for arrival in spread(p, k - 1, True):
            arrival.wait_recv()
        if k < bits:
            for copy in spread(p, k, False):
                start(copy)
        else:
            pltpu.make_async_copy(total.at[p], out[p], o_sem.at[p]).start()

    def vec_stage(i):
        if i == 0:
            v_part.wait_recv()
            v_work[0] = vec[:, core] + v_core[...]
        if 0 < i <= bits:
            copy_to(
                v_work.at[i - 1], v_plane.at[i - 1], v_send.at[i], v_recv.at[i], flip(s, i - 1), f
            ).wait_recv()
            v_work[i] = v_work[i - 1] + v_plane[i - 1]
        if i < bits:
            start(
                copy_to(
                    v_work.at[i], v_plane.at[i], v_send.at[i + 1], v_recv.at[i + 1], flip(s, i), f
                )
            )
        if i == bits:
            for d in range(1, n_z):
                start(
                    copy_to(
                        v_work.at[bits, lax.rem(zed + d, n_z)],
                        v_z.at[d - 1],
                        v_send.at[bits + d],
                        v_recv.at[bits + d],
                        s,
                        to_f[d],
                    )
                )
        if i == bits + 1:
            value = v_work[bits, zed]
            for d in range(1, n_z):
                copy_to(
                    v_work.at[bits, zed],
                    v_z.at[d - 1],
                    v_send.at[bits + d],
                    v_recv.at[bits + d],
                    s,
                    to_f[d],
                ).wait_recv()
                value = value + v_z[d - 1]
            vec_out[...] = value

    n = len(chunks)
    events = []
    for i in range(n):
        events.append((i, 0, functools.partial(stage_core, *chunks[i])))
        for e, k in enumerate(range(bits - 1, -1, -1)):
            events.append((i + 1 + e, 1 + e, functools.partial(stage_plane, *chunks[i], k)))
    for p in range(packs):
        last = (p + 1) * n_z - 1 + bits
        events.append((last + 2, 20, functools.partial(stage_total, p)))
        for k in range(1, bits + 1):
            events.append((last + 2 + k, 20 + k, functools.partial(stage_spread, p, k)))
    for i in range(bits + 2):
        events.append((i + 1, 40, functools.partial(vec_stage, i)))
    for _, _, run in sorted(events, key=lambda e: e[:2]):
        run()
    for p in range(packs):
        pltpu.make_async_copy(total.at[p], out[p], o_sem.at[p]).wait()
    for copy in sent:
        copy.wait_send()


def reduce_all(n_seq, n_fsdp, parts, grads, vec, collective_id):
    packs = len(grads) // 4
    n_z = n_fsdp // 2
    bits = n_seq.bit_length() - 1
    piece = grads[0].shape[2:]
    low, dma, vmem = grads[0].dtype, pltpu.SemaphoreType.DMA, pltpu.VMEM
    vshape = vec.shape[2:]
    return pl.pallas_call(
        functools.partial(reduce_kernel, n_seq, n_fsdp, packs, parts),
        out_shape=[jax.ShapeDtypeStruct((n_seq,) + piece, low) for _ in range(packs)]
        + [jax.ShapeDtypeStruct(vshape, vec.dtype)],
        in_specs=[pl.BlockSpec(memory_space=pl.ANY)] * len(grads)
        + [pl.BlockSpec(memory_space=pltpu.VMEM)],
        out_specs=[pl.BlockSpec(memory_space=pl.ANY)] * packs
        + [pl.BlockSpec(memory_space=pltpu.VMEM)],
        scratch_shapes=[
            vmem((packs, n_z, n_seq) + piece, low),
            vmem((packs, n_z, n_seq) + piece, low),
            vmem((packs, n_z, parts, n_seq - 1) + piece[1:], low),
            vmem((packs, n_z - 1) + piece, low),
            vmem((packs, n_seq) + piece, low),
            vmem((n_z,) + vshape, vec.dtype),
            vmem((bits, n_z) + vshape, vec.dtype),
            vmem((n_z - 1,) + vshape, vec.dtype),
            vmem((bits + 1, n_z) + vshape, vec.dtype),
            dma((packs, n_z, n_seq)),
            dma((packs, n_z, n_seq)),
            dma((packs, n_z, n_seq)),
            dma((packs, n_z, parts, n_seq - 1)),
            dma((packs, n_z, parts, n_seq - 1)),
            dma((packs, n_z)),
            dma((packs, n_z)),
            dma((packs, parts, n_seq - 1)),
            dma((packs, parts, n_seq - 1)),
            dma((bits + n_z,)),
            dma((bits + n_z,)),
            dma((packs,)),
        ],
        compiler_params=pltpu.CompilerParams(
            collective_id=collective_id, has_side_effects=True, vmem_limit_bytes=VMEM_LIMIT
        ),
        name="reduce_grads",
    )(*grads, vec)


def product(left, right):
    return jnp.dot(left, right, preferred_element_type=jnp.float32)


def product_rows(left, right):
    return lax.dot_general(
        left, right, (((0,), (0,)), ((), ())), preferred_element_type=jnp.float32
    )


def product_back(left, right):
    return lax.dot_general(
        left, right, (((1,), (1,)), ((), ())), preferred_element_type=jnp.float32
    )


def gelu_tanh(values):
    return jax.nn.gelu(values, approximate=True)


def normalize(values):
    center = values - jnp.mean(values, axis=-1, keepdims=True)
    factor = lax.rsqrt(jnp.mean(center * center, axis=-1, keepdims=True) + EPSILON)
    return (center * factor, factor)


def norm_back(grad_normed, normed, factor):
    first = jnp.mean(grad_normed, axis=-1, keepdims=True)
    second = jnp.mean(grad_normed * normed, axis=-1, keepdims=True)
    return factor * (grad_normed - first - normed * second)


def wide(values):
    return values.astype(jnp.float32)


def forward_image(items):
    query, keys, values, valid = items
    length, local = query.shape
    heads = local // HD
    scale = HD ** (-0.5)
    query_three = query.reshape(length, heads, HD)
    key_three = keys.reshape(length, heads, HD)
    value_three = values.reshape(length, heads, HD)
    scores = (
        jnp.einsum("qhd,khd->hqk", query_three, key_three, preferred_element_type=jnp.float32)
        * scale
    )
    scores = jnp.where(valid[None, None, :], scores, MASKED)
    highest = jnp.max(scores, axis=-1, keepdims=True)
    logsum = highest + jnp.log(jnp.sum(jnp.exp(scores - highest), axis=-1, keepdims=True))
    attention = jnp.exp(scores - logsum).astype(jnp.bfloat16)
    attended = jnp.einsum(
        "hqk,khd->qhd", attention, value_three, preferred_element_type=jnp.float32
    )
    return (attended.astype(jnp.bfloat16).reshape(length, local), logsum[..., 0])


def backward_image(items):
    query, keys, values, attended, grad_out, logsum, valid = items
    length, local = query.shape
    heads = local // HD
    scale = HD ** (-0.5)
    query, keys, values, attended, grad_out = (
        item.reshape(length, heads, HD) for item in (query, keys, values, attended, grad_out)
    )
    scores = jnp.einsum("qhd,khd->hqk", query, keys, preferred_element_type=jnp.float32) * scale
    scores = jnp.where(valid[None, None, :], scores, MASKED)
    chance = jnp.exp(scores - logsum[:, :, None])
    chance_low = chance.astype(jnp.bfloat16)
    grad_values = jnp.einsum(
        "hqk,qhd->khd", chance_low, grad_out, preferred_element_type=jnp.float32
    )
    grad_chance = jnp.einsum("qhd,khd->hqk", grad_out, values, preferred_element_type=jnp.float32)
    delta = jnp.sum(wide(grad_out) * wide(attended), axis=-1).T
    grad_scores = (chance * (grad_chance - delta[:, :, None]) * scale).astype(jnp.bfloat16)
    grad_query = jnp.einsum("hqk,khd->qhd", grad_scores, keys, preferred_element_type=jnp.float32)
    grad_keys = jnp.einsum("hqk,qhd->khd", grad_scores, query, preferred_element_type=jnp.float32)
    return tuple(
        item.astype(jnp.bfloat16).reshape(length, local)
        for item in (grad_query, grad_keys, grad_values)
    )


def to_heads(tokens):
    return lax.all_to_all(tokens, "seq", split_axis=2, concat_axis=1, tiled=True)


def to_tokens(heads):
    return lax.all_to_all(heads, "seq", split_axis=1, concat_axis=2, tiled=True)


def shards(
    n_seq,
    n_fsdp,
    images,
    key_mask,
    attn_gain,
    attn_shift,
    query_weight,
    key_weight,
    value_weight,
    query_bias,
    value_bias,
    out_weight,
    out_bias,
    mlp_gain,
    mlp_shift,
    inner_weight,
    inner_bias,
    outer_weight,
    outer_bias,
    cotangent,
):
    count, block_len, width = images.shape
    rows = count * block_len
    low = images.dtype
    depth = query_weight.shape[0]
    ff_own = outer_weight.shape[0]
    slack = 4 * depth - ff_own
    bits = n_seq.bit_length() - 1
    piece = 4 * depth // n_seq
    parts = bits if piece % (8 * bits) == 0 else 1
    shape = (parts, piece // parts, width)

    inner_cols = jnp.pad(
        inner_weight.reshape(depth, n_fsdp, ff_own), ((0, 0), (0, 0), (0, slack))
    ).reshape(depth, n_fsdp, 4, depth)
    packed = (
        jnp.stack((query_weight, key_weight, value_weight, out_weight)),
        inner_cols.transpose(2, 0, 1, 3).reshape(4, depth, width),
        jnp.pad(outer_weight, ((0, slack), (0, 0))),
    )
    small = jnp.concatenate(
        (
            attn_gain,
            attn_shift,
            query_bias,
            value_bias,
            out_bias,
            mlp_gain,
            mlp_shift,
            outer_bias,
            inner_bias,
        )
    )
    vec_rows = -(-small.shape[0] // 2048) * 16
    vec = jnp.pad(small, (0, vec_rows * 128 - small.shape[0])).reshape(vec_rows, 128)
    *full, vec_full = gather_all(
        n_seq, n_fsdp, [item.reshape((n_seq,) + shape) for item in packed], vec
    )

    def square(item):
        return (
            item.reshape(4, n_seq // 4, n_fsdp, piece, width)
            .swapaxes(1, 2)
            .reshape(4, width, width)
        )

    w_attn, w_inner, w_outer = (square(item) for item in full)
    w_query, w_key, w_value, w_out = (w_attn[i] for i in range(4))
    flat_vec = wide(vec_full.reshape(n_fsdp, vec_rows * 128))
    gain_attn, shift_attn, b_query, b_value, b_out, gain_mlp, shift_mlp, b_outer = (
        flat_vec[:, i * depth : (i + 1) * depth].reshape(width) for i in range(8)
    )
    b_inner = (
        jnp.pad(flat_vec[:, 8 * depth : 8 * depth + ff_own], ((0, 0), (0, slack)))
        .reshape(n_fsdp, 4, depth)
        .transpose(1, 0, 2)
        .reshape(4, width)
    )

    flat = wide(images.reshape(rows, width))
    normed_one, factor_one = normalize(flat)
    hidden_one = (normed_one * gain_attn + shift_attn).astype(low)
    query = (product(hidden_one, w_query) + b_query).astype(low)
    keys = product(hidden_one, w_key).astype(low)
    values = (product(hidden_one, w_value) + b_value).astype(low)
    tokens = (count, block_len, width)
    query_heads, key_heads, value_heads = (
        to_heads(item.reshape(tokens)) for item in (query, keys, values)
    )
    valid = key_mask > 0
    attended, logsum = lax.map(forward_image, (query_heads, key_heads, value_heads, valid))
    attended_flat = to_tokens(attended).reshape(rows, width)
    second = flat + product(attended_flat, w_out) + b_out
    normed_two, factor_two = normalize(second)
    hidden_two = (normed_two * gain_mlp + shift_mlp).astype(low)
    inner = [product(hidden_two, w_inner[i]) + b_inner[i] for i in range(4)]
    active = [gelu_tanh(item).astype(low) for item in inner]
    outer = sum(product(active[i], w_outer[i]) for i in range(4))
    layer_out = second + outer + b_outer

    upstream = cotangent.reshape(rows, width)
    grad_inner = [
        jax.vjp(gelu_tanh, inner[i])[1](product_back(upstream, w_outer[i]))[0] for i in range(4)
    ]
    grad_inner_low = [item.astype(low) for item in grad_inner]
    grad_hidden_two = sum(product_back(grad_inner_low[i], w_inner[i]) for i in range(4))
    grad_second = wide(upstream) + norm_back(grad_hidden_two * gain_mlp, normed_two, factor_two)
    grad_second_low = grad_second.astype(low)

    grad_attended = product_back(grad_second_low, w_out).astype(low)
    grad_heads = to_heads(grad_attended.reshape(tokens))
    grad_query, grad_keys, grad_values = (
        to_tokens(item).reshape(rows, width)
        for item in lax.map(
            backward_image,
            (query_heads, key_heads, value_heads, attended, grad_heads, logsum, valid),
        )
    )
    grad_hidden_one = (
        product_back(grad_query, w_query)
        + product_back(grad_keys, w_key)
        + product_back(grad_values, w_value)
    )
    images_grad = grad_second + norm_back(grad_hidden_one * gain_attn, normed_one, factor_one)

    squares = [
        product_rows(hidden_one, grad_query),
        product_rows(hidden_one, grad_keys),
        product_rows(hidden_one, grad_values),
        product_rows(attended_flat, grad_second_low),
    ]
    squares += [product_rows(hidden_two, item) for item in grad_inner_low]
    squares += [product_rows(item, upstream) for item in active]
    sums = [
        jnp.sum(grad_hidden_one * normed_one, axis=0),
        jnp.sum(grad_hidden_one, axis=0),
        jnp.sum(wide(grad_query), axis=0),
        jnp.sum(wide(grad_values), axis=0),
        jnp.sum(grad_second, axis=0),
        jnp.sum(grad_hidden_two * normed_two, axis=0),
        jnp.sum(grad_hidden_two, axis=0),
        jnp.sum(wide(upstream), axis=0),
    ]
    inner_sum = (
        jnp.stack([jnp.sum(item, axis=0) for item in grad_inner])
        .reshape(4, n_fsdp, depth)
        .transpose(1, 0, 2)
        .reshape(n_fsdp, 4 * depth)[:, :ff_own]
    )
    vec_grad = jnp.concatenate([item.reshape(n_fsdp, depth) for item in sums] + [inner_sum], axis=1)
    vec_grad = jnp.pad(vec_grad, ((0, 0), (0, vec_rows * 128 - vec_grad.shape[1])))
    *reduced, vec_sum = reduce_all(
        n_seq,
        n_fsdp,
        parts,
        [item.astype(low).reshape((n_fsdp, n_seq // 4) + shape) for item in squares],
        vec_grad.reshape(n_fsdp // 2, 2, vec_rows, 128),
        1,
    )
    attn, inn, out = (wide(item).reshape(4, depth, width) for item in reduced)
    inner_grad = (
        inn.reshape(4, depth, n_fsdp, depth)
        .transpose(1, 2, 0, 3)
        .reshape(depth, n_fsdp, 4 * depth)[:, :, :ff_own]
        .reshape(inner_weight.shape)
    )
    outer_grad = out.reshape(4 * depth, width)[:ff_own]
    sums = vec_sum.reshape(vec_rows * 128)
    small_grads = [sums[i * depth : (i + 1) * depth] for i in range(8)]
    return (
        layer_out.reshape(tokens),
        images_grad.reshape(tokens),
        small_grads[0],
        small_grads[1],
        attn[0],
        attn[1],
        attn[2],
        small_grads[2],
        small_grads[3],
        attn[3],
        small_grads[4],
        small_grads[5],
        small_grads[6],
        inner_grad,
        sums[8 * depth : 8 * depth + ff_own],
        outer_grad,
        small_grads[7],
    )


def solution(mesh):
    vector, matrix, tokens = P("fsdp"), P("fsdp", None), P("fsdp", "seq", None)
    params = (
        vector,
        vector,
        matrix,
        matrix,
        matrix,
        vector,
        vector,
        matrix,
        vector,
        vector,
        vector,
        matrix,
        vector,
        matrix,
        vector,
    )
    return jax.shard_map(
        functools.partial(shards, mesh.shape["seq"], mesh.shape["fsdp"]),
        mesh=mesh,
        in_specs=(tokens, matrix) + params + (tokens,),
        out_specs=(tokens, tokens) + params,
        check_vma=False,
    )
```

```python
import functools

import jax
import jax.numpy as jnp
from jax import lax
from jax.experimental import pallas as pl
from jax.experimental.pallas import tpu as pltpu
from jax.sharding import PartitionSpec as P

HD = 72
EPSILON = 1e-06
MASKED = -1e30
LOG2_E = 1.4426950408889634
MESH = pl.DeviceIdType.MESH
VMEM_LIMIT = 64_000_000
BLOCKS = 4
LOW = jnp.bfloat16
WIDE = jnp.float32


def wide(values):
    return values.astype(WIDE)


def product(left, right):
    return jnp.dot(left, right, preferred_element_type=WIDE)


def product_rows(left, right):
    return lax.dot_general(left, right, (((0,), (0,)), ((), ())), preferred_element_type=WIDE)


def product_back(left, right):
    return lax.dot_general(left, right, (((1,), (1,)), ((), ())), preferred_element_type=WIDE)


def flip(index, bit):
    on = lax.rem(lax.div(index, 1 << bit), 2)
    return index + (1 - 2 * on) * (1 << bit)


def flip_mask(index, mask):
    bit = 0
    while mask >> bit:
        if (mask >> bit) & 1:
            index = flip(index, bit)
        bit += 1
    return index


PLAN = (((0, (0,), 0), (1, (0, 1), 1)), ((1, (0,), 0), (0, (0, 2), 1)))


class Place:
    def __init__(self, n_seq, n_fsdp, depth):
        self.n_seq, self.n_fsdp, self.depth = n_seq, n_fsdp, depth
        self.n_z = n_fsdp // 2
        self.s, self.f = lax.axis_index("seq"), lax.axis_index("fsdp")
        self.core, self.z = lax.rem(self.f, 2), lax.div(self.f, 2)
        self.block = lax.rem(self.s, BLOCKS)
        self.other = self.f + 1 - 2 * self.core
        n_z = self.n_z
        self.to_f = [lax.rem(self.z + d, n_z) * 2 + self.core for d in range(n_z)]
        self.from_f = [lax.rem(self.z - d + n_z, n_z) * 2 + self.core for d in range(n_z)]
        self.to_s = [lax.rem(self.s + d, n_seq) for d in range(n_seq)]
        self.from_s = [lax.rem(self.s - d + n_seq, n_seq) for d in range(n_seq)]
        first = depth // 32 * 16
        self.halves = ((0, first), (first, depth - first))
        self.sent = []

    def greet(self):
        barrier = pltpu.get_barrier_semaphore()
        peers = [(self.s, self.other)]
        peers += [(self.s, f) for f in self.to_f[1:]]
        peers += [(s, self.f) for s in self.to_s[1:]]
        for s, f in peers:
            pl.semaphore_signal(
                barrier, inc=1, device_id={"seq": s, "fsdp": f}, device_id_type=MESH
            )
        pl.semaphore_wait(barrier, len(peers))

    def copy(self, src, dst, sems, index, s, f):
        return pltpu.make_async_remote_copy(
            src_ref=src,
            dst_ref=dst,
            send_sem=sems[0].at[index],
            recv_sem=sems[1].at[index],
            device_id={"seq": s, "fsdp": f},
            device_id_type=MESH,
        )

    def start(self, copies):
        for copy in copies:
            copy.start()
            self.sent.append(copy)

    def finish(self):
        for copy in self.sent:
            copy.wait_send()

    def rows(self, f, half=None):
        offset, size = (0, self.depth) if half is None else self.halves[half]
        return pl.ds(pl.multiple_of(f * self.depth + offset, 8), size)

    def part(self, half):
        return pl.ds(*self.halves[half])


def arrive(copies):
    for copy in copies:
        copy.wait_recv()


class Exchange:
    def __init__(self, place, out, into, sems, local):
        self.place, self.out, self.into, self.sems, self.local = place, out, into, sems, local

    def send(self, i):
        at = self.place
        at.start(
            at.copy(
                self.out.at[i, at.to_s[d]],
                self.into.at[i, at.s],
                self.sems,
                (i, d),
                at.to_s[d],
                at.f,
            )
            for d in range(1, at.n_seq)
        )
        self.keep(i).start()

    def keep(self, i):
        at = self.place
        return pltpu.make_async_copy(
            self.out.at[i, at.s], self.into.at[i, at.s], self.local.at[i]
        )

    def receive(self, i):
        at = self.place
        arrive(
            at.copy(
                self.out.at[i, at.to_s[d]],
                self.into.at[i, at.from_s[d]],
                self.sems,
                (i, d),
                at.to_s[d],
                at.f,
            )
            for d in range(1, at.n_seq)
        )
        self.keep(i).wait()


def heads_of(ref, i, w, head, n_seq):
    rows = slice(head * HD, (head + 1) * HD)
    return jnp.concatenate([ref[i, t, w, rows, :] for t in range(n_seq)], axis=1)


def normalize(values):
    center = values - jnp.mean(values, axis=-1, keepdims=True)
    factor = lax.rsqrt(jnp.mean(center * center, axis=-1, keepdims=True) + EPSILON)
    return (center * factor, factor)


def forward_heads(i, heads, n_seq, qkv, mask, logsum):
    scale = HD ** (-0.5) * LOG2_E
    outs, sums = [], []
    for h in range(heads):
        query, keys, values = (heads_of(qkv, i, w, h, n_seq) for w in range(3))
        scores = product_rows(keys, query) + mask[i]
        highest = jnp.max(scores, axis=0, keepdims=True)
        weights = jnp.exp2((scores - highest) * scale)
        total = jnp.sum(weights, axis=0, keepdims=True)
        outs.append(product(values, (weights * (1.0 / total)).astype(LOW)))
        sums.append(highest * scale + jnp.log2(total))
    logsum[i] = jnp.concatenate(sums, axis=0)
    return jnp.concatenate(outs, axis=0)


def backward_heads(i, heads, n_seq, qkv, attended, grad, mask, logsum):
    scale = HD ** (-0.5)
    grads = [[], [], []]
    for h in range(heads):
        query, keys, values = (heads_of(qkv, i, w, h, n_seq) for w in range(3))
        grad_out = heads_of(grad, i, 0, h, n_seq)
        delta = jnp.sum(
            wide(grad_out) * wide(heads_of(attended, i, 0, h, n_seq)), axis=0, keepdims=True
        )
        scores = product_rows(keys, query) * (scale * LOG2_E)
        chance = jnp.exp2(scores + mask[i] - logsum[i, h : h + 1, :])
        grad_scores = chance * (product_rows(values, grad_out) - delta) * scale
        grads[2].append(product_back(grad_out, chance.astype(LOW)))
        grad_scores = grad_scores.astype(LOW)
        grads[0].append(product(keys, grad_scores))
        grads[1].append(product_back(query, grad_scores))
    return [jnp.concatenate(item, axis=0) for item in grads]


def scatter_tokens(value, n_seq, out, i, w):
    block = value.shape[1] // n_seq
    low = value.astype(LOW)
    for t in range(n_seq):
        out[i, t, w] = low[:, t * block : (t + 1) * block]


def forward_kernel(n_seq, n_fsdp, packs, *refs):
    refs = list(refs)

    def take(n):
        items = refs[:n]
        del refs[:n]
        return items

    images, mask, vec = take(3)
    own = take(packs)
    full = take(packs)
    vec_rows, hidden, attended_flat, logsum, qkv_out, attended_out = take(6)
    weight, vec_full, spread, qkv, attended, attended_in = take(6)
    z_sems, p_sems, c_sems, v_sems, a_sems, b_sems = (take(2) for _ in range(6))
    local, load, a_local, b_local, o_sem = take(5)
    count, block, width = images.shape
    depth = own[0].shape[1]
    group = width // n_seq
    heads = group // HD
    at = Place(n_seq, n_fsdp, depth)
    n_z = at.n_z
    at.greet()

    def vec_copy(src, dst, sem, f):
        return at.copy(src, vec_full.at[dst], v_sems, sem, at.s, f)

    def z_copy(p, d, arriving):
        dst = full[p].at[at.block, at.rows(at.from_f[d] if arriving else at.f)]
        return at.copy(own[p].at[at.block], dst, z_sems, (p, d), at.s, at.to_f[d])

    def plane(p, d, k, arriving):
        for half, steps in enumerate(PLAN):
            bit, masks, slot = steps[k]
            rows = at.rows(at.from_f[d], half)
            for i, m in enumerate(masks):
                src = full[p].at[flip_mask(at.block, m), rows]
                dst = full[p].at[flip_mask(at.block, m ^ (1 << bit)), rows] if arriving else src
                yield at.copy(src, dst, p_sems, (p, d, half, slot + i), flip(at.s, bit), at.f)

    def core_copy(p, d, arriving):
        f = at.from_f[d]
        src = own[p] if d == 0 else full[p].at[:, at.rows(f)]
        dst = full[p].at[:, at.rows(f + 1 - 2 * at.core if arriving else f)]
        return at.copy(src, dst, c_sems, (p, d), at.s, at.other)

    at.start([vec_copy(vec, at.f, d, at.to_f[d]) for d in range(1, n_z)])
    at.start([vec_copy(vec, at.f, 0, at.other)])
    at.start([z_copy(p, d, False) for p in range(packs) for d in range(1, n_z)])
    keep = [
        pltpu.make_async_copy(own[p], full[p].at[:, at.rows(at.f)], local.at[p])
        for p in range(packs)
    ] + [pltpu.make_async_copy(vec, vec_full.at[at.f], local.at[packs])]
    for copy in keep:
        copy.start()
    at.start([core_copy(p, 0, False) for p in range(packs)])
    for d in range(1, n_z):
        arrive([vec_copy(vec, at.from_f[d], d, at.to_f[d])])
        at.start([vec_copy(vec_full.at[at.from_f[d]], at.from_f[d], n_z - 1 + d, at.other)])
    for d in range(n_z):
        sem = n_z - 1 + d if d else 0
        f = at.from_f[d] + 1 - 2 * at.core
        arrive([vec_copy(vec_full.at[f], f, sem, at.other)])
    keep[packs].wait()

    vec_rows[...] = jnp.concatenate([wide(vec_full[f]) for f in range(n_fsdp)], axis=1)
    for i in range(count):
        normed, _ = normalize(wide(images[i]))
        rows = slice(i * block, (i + 1) * block)
        hidden[rows, :] = (normed * vec_rows[0:1, :] + vec_rows[1:2, :]).astype(LOW)

    def from_z(p, d):
        arrive([z_copy(p, d, True)])
        at.start(plane(p, d, 0, False))

    def second_step(p):
        for d in range(1, n_z):
            arrive(plane(p, d, 0, True))
            at.start(plane(p, d, 1, False))

    def to_core(p, d):
        arrive(plane(p, d, 1, True))
        at.start([core_copy(p, d, False)])

    def weight_load(w):
        return pltpu.make_async_copy(full[0].at[w], weight.at[w % 2], load.at[w % 2])

    send_heads = Exchange(at, spread, qkv, a_sems, a_local)
    send_tokens = Exchange(at, attended, attended_in, b_sems, b_local)

    for d in range(1, n_z):
        from_z(0, d)
    second_step(0)
    for d in range(1, n_z):
        from_z(1, d)
        to_core(0, d)
    for d in range(n_z):
        arrive([core_copy(0, d, True)])
    keep[0].wait()
    weight_load(0).start()
    for w in range(3):
        if w < 2:
            weight_load(w + 1).start()
        weight_load(w).wait()
        value = product(hidden[...], weight[w % 2])
        if w != 1:
            value = value + vec_rows[2 + w // 2 : 3 + w // 2, :]
        value = value.T.astype(LOW)
        for i in range(count):
            for t in range(n_seq):
                spread[i, t, w] = value[
                    t * group : (t + 1) * group, i * block : (i + 1) * block
                ]
    for i in range(count):
        send_heads.send(i)
    second_step(1)
    for d in range(1, n_z):
        from_z(2, d)
    for i in range(count):
        send_heads.receive(i)
        scatter_tokens(
            forward_heads(i, heads, n_seq, qkv, mask, logsum), n_seq, attended, i, 0
        )
        send_tokens.send(i)
        if i == 0:
            for d in range(1, n_z):
                to_core(1, d)
            second_step(2)
    saves = [
        pltpu.make_async_copy(qkv, qkv_out, o_sem.at[0]),
        pltpu.make_async_copy(attended, attended_out, o_sem.at[1]),
    ]
    for copy in saves:
        copy.start()
    for d in range(1, n_z):
        to_core(2, d)
    for i in range(count):
        send_tokens.receive(i)
        features = jnp.concatenate([attended_in[i, t, 0] for t in range(n_seq)], axis=0)
        attended_flat[i * block : (i + 1) * block, :] = wide(features).T.astype(LOW)
    for p in range(packs):
        if p > 0:
            keep[p].wait()
            for d in range(n_z):
                arrive([core_copy(p, d, True)])
    for copy in saves:
        copy.wait()
    at.finish()


def forward_all(n_seq, n_fsdp, images, mask, vec, packed):
    packs = len(packed)
    count, block, width = images.shape
    length = mask.shape[1]
    n_z, group = n_fsdp // 2, width // n_seq
    heads = group // HD
    dma, vmem, any_space = pltpu.SemaphoreType.DMA, pltpu.VMEM, pl.BlockSpec(memory_space=pl.ANY)
    in_vmem = pl.BlockSpec(memory_space=pltpu.VMEM)
    shape = jax.ShapeDtypeStruct
    qkv = (count, n_seq, 3, group, block)
    att = (count, n_seq, 1, group, block)
    pair = lambda *dims: [dma(dims), dma(dims)]
    return pl.pallas_call(
        functools.partial(forward_kernel, n_seq, n_fsdp, packs),
        out_shape=[shape((BLOCKS, width, width), LOW) for _ in range(packs)]
        + [
            shape((vec.shape[0], width), WIDE),
            shape((count * block, width), LOW),
            shape((count * block, width), LOW),
            shape((count, heads, length), WIDE),
            shape(qkv, LOW),
            shape(att, LOW),
        ],
        in_specs=[in_vmem] * (3 + packs),
        out_specs=[any_space] * packs + [in_vmem] * 4 + [any_space] * 2,
        scratch_shapes=[
            vmem((2, width, width), LOW),
            vmem((n_fsdp,) + vec.shape, LOW),
            vmem(qkv, LOW),
            vmem(qkv, LOW),
            vmem(att, LOW),
            vmem(att, LOW),
            *pair(packs, n_z),
            *pair(packs, n_z, 2, BLOCKS - 1),
            *pair(packs, n_z),
            *pair(2 * n_z - 1),
            *pair(count, n_seq),
            *pair(count, n_seq),
            dma((packs + 1,)),
            dma((2,)),
            dma((count,)),
            dma((count,)),
            dma((2,)),
        ],
        compiler_params=pltpu.CompilerParams(
            collective_id=0, has_side_effects=True, vmem_limit_bytes=VMEM_LIMIT
        ),
        name="forward_attention",
    )(images, mask, vec, *packed)


def add_rows(target, term, start, size):
    step = 16 if start % 16 == 0 and size % 16 == 0 else 8

    def body(i, _):
        rows = pl.ds(pl.multiple_of(start + i * step, step), step)
        target[rows, :] = (wide(target[rows, :]) + wide(term[rows, :])).astype(LOW)
        return 0

    lax.fori_loop(0, size // step, body, 0)


class Reduction:
    SCRATCH = 14

    @staticmethod
    def scratch(n_seq, n_fsdp, packs, depth, width):
        n_z, upper = n_fsdp // 2, n_seq.bit_length() - 3
        dma, vmem = pltpu.SemaphoreType.DMA, pltpu.VMEM
        piece = (depth, width)
        pair = lambda *dims: [dma(dims), dma(dims)]
        return [
            vmem((packs, n_z, BLOCKS) + piece, LOW),
            vmem((packs, n_z, BLOCKS) + piece, LOW),
            vmem((packs, n_z, BLOCKS - 1) + piece, LOW),
            vmem((packs, n_z - 1) + piece, LOW),
            vmem((packs, BLOCKS) + piece, LOW),
            vmem((max(upper, 1), packs, n_z, BLOCKS) + (piece if upper else (8, 128)), LOW),
            dma((packs, n_z, BLOCKS)),
            dma((packs,)),
            *pair(packs, n_z, BLOCKS),
            *pair(packs, n_z, 2, BLOCKS - 1),
            *pair(packs, n_z),
            *pair(packs, 2, BLOCKS - 1),
            *pair(max(upper, 1), packs, n_z),
        ]

    def __init__(self, at, packs, grads, out, scratch):
        self.at, self.packs, self.grads, self.out = at, packs, grads, out
        (
            self.held,
            self.core_in,
            self.plane_in,
            self.z_in,
            self.total,
            self.upper_in,
            self.load_sem,
            self.out_sem,
            *sems,
        ) = scratch
        self.c_sems, self.p_sems, self.z_sems, self.g_sems, self.u_sems = (
            sems[2 * i : 2 * i + 2] for i in range(5)
        )
        self.upper = at.n_seq.bit_length() - 3

    def target_z(self, t):
        return lax.rem(self.at.z + t + 1, self.at.n_z)

    def load(self, p, t):
        rows = self.at.rows(2 * self.target_z(t) + self.at.core)
        return [
            pltpu.make_async_copy(
                self.grads[p][q].at[rows], self.held.at[p, t, q], self.load_sem.at[p, t, q]
            )
            for q in range(BLOCKS)
        ]

    def to_partner(self, p, t):
        at = self.at
        rows = at.rows(2 * self.target_z(t) + 1 - at.core)
        return [
            at.copy(
                self.grads[p][q].at[rows],
                self.core_in.at[p, t, q],
                self.c_sems,
                (p, t, q),
                at.s,
                at.other,
            )
            for q in range(BLOCKS)
        ]

    def start(self, p, t):
        self.at.start(self.to_partner(p, t))
        for copy in self.load(p, t):
            copy.start()

    def plane(self, p, t, k):
        at = self.at
        for half, steps in enumerate(PLAN):
            bit, masks, slot = steps[k]
            for i, m in enumerate(masks):
                src = self.held.at[p, t, flip_mask(at.block, m ^ (1 << bit)), at.part(half)]
                dst = self.plane_in.at[p, t, slot + i, at.part(half)]
                yield at.copy(
                    src, dst, self.p_sems, (p, t, half, slot + i), flip(at.s, bit), at.f
                )

    def z_copy(self, p, t):
        at = self.at
        return at.copy(
            self.held.at[p, t, at.block],
            self.z_in.at[p, t],
            self.z_sems,
            (p, t),
            at.s,
            2 * self.target_z(t) + at.core,
        )

    def up_copy(self, u, p, t):
        at = self.at
        return at.copy(
            self.held.at[p, t],
            self.upper_in.at[u, p, t],
            self.u_sems,
            (u, p, t),
            flip(at.s, 2 + u),
            at.f,
        )

    def spread(self, p, k, arriving):
        at = self.at
        for half, steps in enumerate(PLAN):
            bit, masks, slot = steps[k]
            for i, m in enumerate(masks):
                src = self.total.at[p, flip_mask(at.block, m), at.part(half)]
                dst = self.total.at[p, flip_mask(at.block, m ^ (1 << bit)), at.part(half)]
                yield at.copy(
                    src,
                    dst if arriving else src,
                    self.g_sems,
                    (p, half, slot + i),
                    flip(at.s, bit),
                    at.f,
                )

    def stage_core(self, p, t):
        for copy in self.load(p, t):
            copy.wait()
        arrive(self.to_partner(p, t))

        def body(q, _):
            add_rows(self.held.at[p, t, q], self.core_in.at[p, t, q], 0, self.at.depth)
            return 0

        lax.fori_loop(0, BLOCKS, body, 0)
        for u in range(self.upper):
            copy = self.up_copy(u, p, t)
            copy.start()
            copy.wait()

            def upper_body(q, _, u=u):
                add_rows(self.held.at[p, t, q], self.upper_in.at[u, p, t, q], 0, self.at.depth)
                return 0

            lax.fori_loop(0, BLOCKS, upper_body, 0)
        self.at.start(self.plane(p, t, 1))

    def stage_plane(self, p, t, k):
        arrive(self.plane(p, t, k))
        for half, steps in enumerate(PLAN):
            _, masks, slot = steps[k]
            for i, m in enumerate(masks):
                add_rows(
                    self.held.at[p, t, flip_mask(self.at.block, m)],
                    self.plane_in.at[p, t, slot + i],
                    *self.at.halves[half],
                )
        if k > 0:
            self.at.start(self.plane(p, t, k - 1))
        elif t < self.at.n_z - 1:
            self.at.start([self.z_copy(p, t)])

    def stage_total(self, p):
        last = self.at.n_z - 1
        arrive(self.z_copy(p, t) for t in range(last))
        step = 16 if self.at.depth % 16 == 0 else 8

        def body(i, _):
            rows = pl.ds(pl.multiple_of(i * step, step), step)
            value = wide(self.held[p, last, self.at.block, rows, :])
            for t in range(last):
                value = value + wide(self.z_in[p, t, rows, :])
            self.total[p, self.at.block, rows, :] = value.astype(LOW)
            return 0

        lax.fori_loop(0, self.at.depth // step, body, 0)
        self.at.start(self.spread(p, 0, False))

    def stage_spread(self, p, k):
        arrive(self.spread(p, k - 1, True))
        if k < 2:
            self.at.start(self.spread(p, k, False))
        else:
            self.save(p).start()

    def save(self, p):
        return pltpu.make_async_copy(self.total.at[p], self.out[p], self.out_sem.at[p])

    def events(self):
        n_z, out = self.at.n_z, []
        for i, (p, t) in enumerate((p, t) for p in range(self.packs) for t in range(n_z)):
            out.append((i, 0, functools.partial(self.stage_core, p, t)))
            out.append((i + 1, 1, functools.partial(self.stage_plane, p, t, 1)))
            out.append((i + 2, 2, functools.partial(self.stage_plane, p, t, 0)))
        for p in range(self.packs):
            last = (p + 1) * n_z + 1
            out.append((last + 1.5, 3, functools.partial(self.stage_total, p)))
            out.append((last + 2.5, 4, functools.partial(self.stage_spread, p, 1)))
            out.append((last + 3.5, 5, functools.partial(self.stage_spread, p, 2)))
        return out

    def finish(self):
        for p in range(self.packs):
            self.save(p).wait()


def run_events(events):
    for _, _, call in sorted(events, key=lambda e: e[:2]):
        call()


def backward_kernel(n_seq, n_fsdp, packs, *refs):
    refs = list(refs)

    def take(n):
        items = refs[:n]
        del refs[:n]
        return items

    grads = [take(BLOCKS) for _ in range(packs)]
    grad_flat, mask, logsum, qkv, attended = take(5)
    out = take(packs)
    (grad_out,) = take(1)
    grad_spread, grad_heads, back_spread, back_in = take(4)
    a_sems, b_sems = take(2), take(2)
    a_local, b_local = take(2)
    count, _, _, group, block = qkv.shape
    width = grad_flat.shape[1]
    heads = group // HD
    at = Place(n_seq, n_fsdp, width // n_fsdp)
    reduction = Reduction(at, packs, grads, out, refs)
    at.greet()
    send_heads = Exchange(at, grad_spread, grad_heads, a_sems, a_local)
    send_tokens = Exchange(at, back_spread, back_in, b_sems, b_local)
    for i in range(count):
        value = wide(grad_flat[i * block : (i + 1) * block, :]).T.astype(LOW)
        for t in range(n_seq):
            grad_spread[i, t, 0] = value[t * group : (t + 1) * group]
        send_heads.send(i)
    for p in range(packs):
        for t in range(at.n_z):
            reduction.start(p, t)

    def image(i):
        send_heads.receive(i)
        for w, value in enumerate(
            backward_heads(i, heads, n_seq, qkv, attended, grad_heads, mask, logsum)
        ):
            scatter_tokens(value, n_seq, back_spread, i, w)
        send_tokens.send(i)

    def collect(i):
        send_tokens.receive(i)
        for w in range(3):
            features = jnp.concatenate([back_in[i, t, w] for t in range(n_seq)], axis=0)
            grad_out[w, i * block : (i + 1) * block, :] = wide(features).T.astype(LOW)

    events = reduction.events()
    for i in range(count):
        events.append((1 + i, 10, functools.partial(image, i)))
        events.append((5 + i, 11, functools.partial(collect, i)))
    run_events(events)
    reduction.finish()
    at.finish()


def backward_all(n_seq, n_fsdp, squares, grad_flat, mask, logsum, qkv, attended):
    packs = len(squares) // BLOCKS
    width = grad_flat.shape[1]
    depth = width // n_fsdp
    count = qkv.shape[0]
    any_space = pl.BlockSpec(memory_space=pl.ANY)
    in_vmem = pl.BlockSpec(memory_space=pltpu.VMEM)
    dma, vmem, shape = pltpu.SemaphoreType.DMA, pltpu.VMEM, jax.ShapeDtypeStruct
    pair = lambda *dims: [dma(dims), dma(dims)]
    return pl.pallas_call(
        functools.partial(backward_kernel, n_seq, n_fsdp, packs),
        out_shape=[shape((BLOCKS, depth, width), LOW) for _ in range(packs)]
        + [shape((3,) + grad_flat.shape, LOW)],
        in_specs=[any_space] * len(squares) + [in_vmem] * 5,
        out_specs=[any_space] * packs + [in_vmem],
        scratch_shapes=[
            vmem(attended.shape, LOW),
            vmem(attended.shape, LOW),
            vmem(qkv.shape, LOW),
            vmem(qkv.shape, LOW),
            *pair(count, n_seq),
            *pair(count, n_seq),
            dma((count,)),
            dma((count,)),
            *Reduction.scratch(n_seq, n_fsdp, packs, depth, width),
        ],
        compiler_params=pltpu.CompilerParams(
            collective_id=1, has_side_effects=True, vmem_limit_bytes=VMEM_LIMIT
        ),
        name="backward_attention",
    )(*squares, grad_flat, mask, logsum, qkv, attended)


def reduce_kernel(n_seq, n_fsdp, packs, *refs):
    refs = list(refs)

    def take(n):
        items = refs[:n]
        del refs[:n]
        return items

    grads = [take(BLOCKS) for _ in range(packs)]
    (vec,) = take(1)
    out = take(packs)
    (vec_out,) = take(1)
    work, came, z_came = take(3)
    v_sems = take(2)
    width = vec.shape[1]
    depth = width // n_fsdp
    at = Place(n_seq, n_fsdp, depth)
    n_z, bits = at.n_z, n_seq.bit_length() - 1
    reduction = Reduction(at, packs, grads, out, refs)
    at.greet()

    def vec_copy(i):
        src = vec if i == 0 else work.at[i - 1]
        peer = (at.s, at.other) if i == 0 else (flip(at.s, i - 1), at.f)
        return at.copy(src, came.at[i], v_sems, i, *peer)

    def vec_z(d):
        return at.copy(
            work.at[bits], z_came.at[lax.rem(at.z, n_z)], v_sems, bits + d, at.s, at.to_f[d]
        )

    def vec_stage(i):
        arrive([vec_copy(i)])
        work[i] = (vec[...] if i == 0 else work[i - 1]) + came[i]
        if i < bits:
            at.start([vec_copy(i + 1)])
        else:
            at.start([vec_z(d) for d in range(1, n_z)])

    def vec_last():
        for d in range(1, n_z):
            arrive(
                [
                    at.copy(
                        work.at[bits],
                        z_came.at[lax.div(at.from_f[d], 2)],
                        v_sems,
                        bits + d,
                        at.s,
                        at.to_f[d],
                    )
                ]
            )
        value = work[bits]
        for d in range(1, n_z):
            value = value + z_came[lax.div(at.from_f[d], 2)]
        for f in range(n_fsdp):

            @pl.when(at.f == f)
            def _(f=f):
                vec_out[...] = value[:, f * depth : (f + 1) * depth]

    at.start([vec_copy(0)])
    for p in range(packs):
        for t in range(n_z):
            reduction.start(p, t)
    events = reduction.events()
    for i in range(bits + 1):
        events.append((i, 20, functools.partial(vec_stage, i)))
    events.append((bits + 1, 20, vec_last))
    run_events(events)
    reduction.finish()
    at.finish()


def reduce_all(n_seq, n_fsdp, squares, vec):
    packs = len(squares) // BLOCKS
    width = vec.shape[1]
    depth = width // n_fsdp
    n_z, bits = n_fsdp // 2, n_seq.bit_length() - 1
    any_space = pl.BlockSpec(memory_space=pl.ANY)
    in_vmem = pl.BlockSpec(memory_space=pltpu.VMEM)
    dma, vmem, shape = pltpu.SemaphoreType.DMA, pltpu.VMEM, jax.ShapeDtypeStruct
    return pl.pallas_call(
        functools.partial(reduce_kernel, n_seq, n_fsdp, packs),
        out_shape=[shape((BLOCKS, depth, width), LOW) for _ in range(packs)]
        + [shape((vec.shape[0], depth), WIDE)],
        in_specs=[any_space] * len(squares) + [in_vmem],
        out_specs=[any_space] * packs + [in_vmem],
        scratch_shapes=[
            vmem((bits + 1,) + vec.shape, WIDE),
            vmem((bits + 1,) + vec.shape, WIDE),
            vmem((n_z,) + vec.shape, WIDE),
            dma((bits + n_z,)),
            dma((bits + n_z,)),
            *Reduction.scratch(n_seq, n_fsdp, packs, depth, width),
        ],
        compiler_params=pltpu.CompilerParams(
            collective_id=2, has_side_effects=True, vmem_limit_bytes=VMEM_LIMIT
        ),
        name="reduce_grads",
    )(*squares, vec)


def gelu_tanh(values):
    return jax.nn.gelu(values, approximate=True)


def norm_back(grad_normed, normed, factor):
    first = jnp.mean(grad_normed, axis=-1, keepdims=True)
    second = jnp.mean(grad_normed * normed, axis=-1, keepdims=True)
    return factor * (grad_normed - first - normed * second)


def shards(
    n_seq,
    n_fsdp,
    images,
    key_mask,
    attn_gain,
    attn_shift,
    query_weight,
    key_weight,
    value_weight,
    query_bias,
    value_bias,
    out_weight,
    out_bias,
    mlp_gain,
    mlp_shift,
    inner_weight,
    inner_bias,
    outer_weight,
    outer_bias,
    cotangent,
):
    count, block_len, width = images.shape
    rows = count * block_len
    depth = query_weight.shape[0]
    ff_own = outer_weight.shape[0]
    slack = BLOCKS * depth - ff_own

    inner_cols = jnp.pad(
        inner_weight.reshape(depth, n_fsdp, ff_own), ((0, 0), (0, 0), (0, slack))
    ).reshape(depth, n_fsdp, BLOCKS, depth)
    packed = (
        jnp.stack((query_weight, key_weight, value_weight, out_weight)),
        inner_cols.transpose(2, 0, 1, 3).reshape(BLOCKS, depth, width),
        jnp.pad(outer_weight, ((0, slack), (0, 0))).reshape(BLOCKS, depth, width),
    )
    small = [
        attn_gain,
        attn_shift,
        query_bias,
        value_bias,
        out_bias,
        mlp_gain,
        mlp_shift,
        outer_bias,
    ]
    vec = jnp.concatenate(
        [item.reshape(1, depth) for item in small]
        + [jnp.pad(inner_bias, (0, slack + BLOCKS * depth)).reshape(2 * BLOCKS, depth)]
    )
    mask = jnp.where(key_mask > 0, 0.0, MASKED).astype(WIDE)[:, :, None]
    *full, vecs, hidden_one, attended_flat, logsum, qkv, attended = forward_all(
        n_seq, n_fsdp, images, mask, vec, packed
    )
    w_attn, w_inner, w_outer = full
    w_query, w_key, w_value, w_out = (w_attn[i] for i in range(BLOCKS))
    gain_attn, _, _, _, b_out, gain_mlp, shift_mlp, b_outer = (vecs[i] for i in range(8))
    b_inner = [vecs[8 + i] for i in range(BLOCKS)]

    flat = wide(images.reshape(rows, width))
    second = flat + product(attended_flat, w_out) + b_out
    normed_two, factor_two = normalize(second)
    hidden_two = (normed_two * gain_mlp + shift_mlp).astype(LOW)
    inner = [product(hidden_two, w_inner[i]) + b_inner[i] for i in range(BLOCKS)]
    active = [gelu_tanh(item).astype(LOW) for item in inner]
    outer = sum(product(active[i], w_outer[i]) for i in range(BLOCKS))
    layer_out = second + outer + b_outer

    upstream = cotangent.reshape(rows, width)
    grad_inner = [
        jax.vjp(gelu_tanh, inner[i])[1](product_back(upstream, w_outer[i]))[0]
        for i in range(BLOCKS)
    ]
    grad_inner_low = [item.astype(LOW) for item in grad_inner]
    grad_hidden_two = sum(product_back(grad_inner_low[i], w_inner[i]) for i in range(BLOCKS))
    grad_second = wide(upstream) + norm_back(grad_hidden_two * gain_mlp, normed_two, factor_two)
    grad_second_low = grad_second.astype(LOW)

    grad_attended = product_back(grad_second_low, w_out).astype(LOW)
    mlp_squares = [product_rows(item, upstream).astype(LOW) for item in active]
    mlp_squares += [product_rows(hidden_two, item).astype(LOW) for item in grad_inner_low]
    sum_outer, sum_inner, grad_qkv = backward_all(
        n_seq, n_fsdp, mlp_squares, grad_attended, mask, logsum, qkv, attended
    )
    grad_query, grad_keys, grad_values = (grad_qkv[i] for i in range(3))
    grad_hidden_one = (
        product_back(grad_query, w_query)
        + product_back(grad_keys, w_key)
        + product_back(grad_values, w_value)
    )
    normed_one, factor_one = normalize(flat)
    images_grad = grad_second + norm_back(grad_hidden_one * gain_attn, normed_one, factor_one)

    squares = [
        product_rows(hidden_one, grad_query),
        product_rows(hidden_one, grad_keys),
        product_rows(hidden_one, grad_values),
        product_rows(attended_flat, grad_second_low),
    ]
    sums = [
        jnp.sum(grad_hidden_one * normed_one, axis=0),
        jnp.sum(grad_hidden_one, axis=0),
        jnp.sum(wide(grad_query), axis=0),
        jnp.sum(wide(grad_values), axis=0),
        jnp.sum(grad_second, axis=0),
        jnp.sum(grad_hidden_two * normed_two, axis=0),
        jnp.sum(grad_hidden_two, axis=0),
        jnp.sum(wide(upstream), axis=0),
    ] + [jnp.sum(item, axis=0) for item in grad_inner]
    vec_grad = jnp.stack(sums + [jnp.zeros_like(sums[0])] * BLOCKS)
    sum_attn, vec_sum = reduce_all(
        n_seq, n_fsdp, [item.astype(LOW) for item in squares], vec_grad
    )
    attn = wide(sum_attn)
    inner_grad = (
        sum_inner.reshape(BLOCKS, depth, n_fsdp, depth)
        .transpose(1, 2, 0, 3)
        .reshape(depth, n_fsdp, BLOCKS * depth)[:, :, :ff_own]
        .reshape(inner_weight.shape)
        .astype(WIDE)
    )
    outer_grad = wide(sum_outer.reshape(BLOCKS * depth, width)[:ff_own])
    return (
        layer_out.reshape(count, block_len, width),
        images_grad.reshape(count, block_len, width),
        vec_sum[0],
        vec_sum[1],
        attn[0],
        attn[1],
        attn[2],
        vec_sum[2],
        vec_sum[3],
        attn[3],
        vec_sum[4],
        vec_sum[5],
        vec_sum[6],
        inner_grad,
        vec_sum[8 : 8 + BLOCKS].reshape(BLOCKS * depth)[:ff_own],
        outer_grad,
        vec_sum[7],
    )


def solution(mesh):
    vector, matrix, tokens = P("fsdp"), P("fsdp", None), P("fsdp", "seq", None)
    params = (
        vector,
        vector,
        matrix,
        matrix,
        matrix,
        vector,
        vector,
        matrix,
        vector,
        vector,
        vector,
        matrix,
        vector,
        matrix,
        vector,
    )
    return jax.shard_map(
        functools.partial(shards, mesh.shape["seq"], mesh.shape["fsdp"]),
        mesh=mesh,
        in_specs=(tokens, matrix) + params + (tokens,),
        out_specs=(tokens, tokens) + params,
        check_vma=False,
    )
```

```python
import functools

import jax
import jax.numpy as jnp
from jax import lax
from jax.experimental import pallas as pl
from jax.experimental.pallas import tpu as pltpu
from jax.sharding import PartitionSpec as P

HD = 72
EPSILON = 1e-06
MASKED = -1e30
LOG2_E = 1.4426950408889634
MESH = pl.DeviceIdType.MESH
VMEM_LIMIT = 67_000_000
BLOCKS = 4
LOW = jnp.bfloat16
WIDE = jnp.float32


def wide(values):
    return values.astype(WIDE)


def product(left, right):
    return jnp.dot(left, right, preferred_element_type=WIDE)


def product_rows(left, right):
    return lax.dot_general(left, right, (((0,), (0,)), ((), ())), preferred_element_type=WIDE)


def product_back(left, right):
    return lax.dot_general(left, right, (((1,), (1,)), ((), ())), preferred_element_type=WIDE)


def flip(index, bit):
    on = lax.rem(lax.div(index, 1 << bit), 2)
    return index + (1 - 2 * on) * (1 << bit)


def flip_mask(index, mask):
    bit = 0
    while mask >> bit:
        if (mask >> bit) & 1:
            index = flip(index, bit)
        bit += 1
    return index


PLAN = (((0, (0,), 0), (1, (0, 1), 1)), ((1, (0,), 0), (0, (0, 2), 1)))


class Place:
    def __init__(self, n_seq, n_fsdp, depth):
        self.n_seq, self.n_fsdp, self.depth = n_seq, n_fsdp, depth
        self.n_z = n_fsdp // 2
        self.s, self.f = lax.axis_index("seq"), lax.axis_index("fsdp")
        self.core, self.z = lax.rem(self.f, 2), lax.div(self.f, 2)
        self.block = lax.rem(self.s, BLOCKS)
        self.other = self.f + 1 - 2 * self.core
        n_z = self.n_z
        self.to_f = [lax.rem(self.z + d, n_z) * 2 + self.core for d in range(n_z)]
        self.from_f = [lax.rem(self.z - d + n_z, n_z) * 2 + self.core for d in range(n_z)]
        self.to_s = [lax.rem(self.s + d, n_seq) for d in range(n_seq)]
        self.from_s = [lax.rem(self.s - d + n_seq, n_seq) for d in range(n_seq)]
        first = depth // 32 * 16
        self.halves = ((0, first), (first, depth - first))
        self.sent = []

    def greet(self):
        barrier = pltpu.get_barrier_semaphore()
        peers = [(self.s, self.other)]
        peers += [(self.s, f) for f in self.to_f[1:]]
        peers += [(s, self.f) for s in self.to_s[1:]]
        for s, f in peers:
            pl.semaphore_signal(
                barrier, inc=1, device_id={"seq": s, "fsdp": f}, device_id_type=MESH
            )
        pl.semaphore_wait(barrier, len(peers))

    def copy(self, src, dst, sems, index, s, f):
        return pltpu.make_async_remote_copy(
            src_ref=src,
            dst_ref=dst,
            send_sem=sems[0].at[index],
            recv_sem=sems[1].at[index],
            device_id={"seq": s, "fsdp": f},
            device_id_type=MESH,
        )

    def start(self, copies):
        for copy in copies:
            copy.start()
            self.sent.append(copy)

    def finish(self):
        for copy in self.sent:
            copy.wait_send()

    def rows(self, f, half=None):
        offset, size = (0, self.depth) if half is None else self.halves[half]
        return pl.ds(pl.multiple_of(f * self.depth + offset, 8), size)

    def part(self, half):
        return pl.ds(*self.halves[half])


def arrive(copies):
    for copy in copies:
        copy.wait_recv()


class Exchange:
    def __init__(self, place, out, into, sems, local):
        self.place, self.out, self.into, self.sems, self.local = place, out, into, sems, local

    def send(self, i):
        at = self.place
        at.start(
            at.copy(
                self.out.at[i, at.to_s[d]],
                self.into.at[i, at.s],
                self.sems,
                (i, d),
                at.to_s[d],
                at.f,
            )
            for d in range(1, at.n_seq)
        )
        self.keep(i).start()

    def keep(self, i):
        at = self.place
        return pltpu.make_async_copy(
            self.out.at[i, at.s], self.into.at[i, at.s], self.local.at[i]
        )

    def receive(self, i):
        at = self.place
        arrive(
            at.copy(
                self.out.at[i, at.to_s[d]],
                self.into.at[i, at.from_s[d]],
                self.sems,
                (i, d),
                at.to_s[d],
                at.f,
            )
            for d in range(1, at.n_seq)
        )
        self.keep(i).wait()


def heads_of(ref, w, head, n_seq):
    rows = slice(head * HD, (head + 1) * HD)
    return jnp.concatenate([ref[t, w, rows, :] for t in range(n_seq)], axis=1)


def normalize(values):
    center = values - jnp.mean(values, axis=-1, keepdims=True)
    factor = lax.rsqrt(jnp.mean(center * center, axis=-1, keepdims=True) + EPSILON)
    return (center * factor, factor)


def norm_back(grad_normed, normed, factor):
    first = jnp.mean(grad_normed, axis=-1, keepdims=True)
    second = jnp.mean(grad_normed * normed, axis=-1, keepdims=True)
    return factor * (grad_normed - first - normed * second)


GELU_SCALE = 0.7978845608028654
GELU_CUBE = 0.044715


def gelu(u):
    return 0.5 * u * (1.0 + jnp.tanh(GELU_SCALE * (u + GELU_CUBE * (u * u * u))))


def gelu_slope(u):
    square = u * u
    bent = jnp.tanh(GELU_SCALE * (u + GELU_CUBE * (u * square)))
    inner = GELU_SCALE * (1.0 + 3.0 * GELU_CUBE * square)
    return 0.5 * (1.0 + bent) + 0.5 * u * (1.0 - bent * bent) * inner


def row_loop(count, body, carry=0, step=16):
    step = step if count % step == 0 else 8
    return lax.fori_loop(
        0,
        count // step,
        lambda i, kept: body(pl.ds(pl.multiple_of(i * step, step), step), kept),
        carry,
    )


def fold(values):
    return sum(values[8 * i : 8 * i + 8] for i in range(values.shape[0] // 8))


def column_sum(kept):
    return jnp.sum(kept, axis=0, keepdims=True)


def tall_product(left, right, out):
    width = left.shape[1]
    tile = 384 if width % 384 == 0 else width

    def body(i, _):
        cols = pl.ds(pl.multiple_of(i * tile, 128), tile)
        out[cols, :] = product_rows(left[:, cols], right[...]).astype(LOW)
        return 0

    lax.fori_loop(0, width // tile, body, 0)


def pieces_to_columns(read, n_fsdp, size, width):
    parts = []
    for f in range(n_fsdp):
        piece = read(f)
        if size < width:
            piece = jnp.concatenate(
                [piece, jnp.zeros((piece.shape[0], width - size), piece.dtype)], axis=1
            )
        parts.append(piece)
    return jnp.concatenate(parts, axis=1)


def forward_heads(i, heads, n_seq, qkv, mask, logsum):
    scale = HD ** (-0.5) * LOG2_E
    outs, sums = [], []
    for h in range(heads):
        query, keys, values = (heads_of(qkv, w, h, n_seq) for w in range(3))
        scores = product_rows(keys, query) + mask[i]
        highest = jnp.max(scores, axis=0, keepdims=True)
        weights = jnp.exp2((scores - highest) * scale)
        total = jnp.sum(weights, axis=0, keepdims=True)
        outs.append(product(values, (weights * (1.0 / total)).astype(LOW)))
        sums.append(highest * scale + jnp.log2(total))
    logsum[i] = jnp.concatenate(sums, axis=0)
    return jnp.concatenate(outs, axis=0)


def backward_heads(i, heads, n_seq, qkv, attended, grad, mask, logsum):
    scale = HD ** (-0.5)
    grads = [[], [], []]
    for h in range(heads):
        query, keys, values = (heads_of(qkv, w, h, n_seq) for w in range(3))
        grad_out = heads_of(grad, 0, h, n_seq)
        delta = jnp.sum(
            wide(grad_out) * wide(heads_of(attended, 0, h, n_seq)), axis=0, keepdims=True
        )
        scores = product_rows(keys, query) * (scale * LOG2_E)
        chance = jnp.exp2(scores + mask[i] - logsum[i, h : h + 1, :])
        grad_scores = chance * (product_rows(values, grad_out) - delta) * scale
        grads[2].append(product_back(grad_out, chance.astype(LOW)))
        grad_scores = grad_scores.astype(LOW)
        grads[0].append(product(keys, grad_scores))
        grads[1].append(product_back(query, grad_scores))
    return [jnp.concatenate(item, axis=0) for item in grads]


def scatter_tokens(value, n_seq, out, i, w):
    block = value.shape[1] // n_seq
    low = value.astype(LOW)
    for t in range(n_seq):
        out[i, t, w] = low[:, t * block : (t + 1) * block]


def forward_kernel(n_seq, n_fsdp, packs, *refs):
    refs = list(refs)

    def take(n):
        items = refs[:n]
        del refs[:n]
        return items

    images, mask, vec, inner_own = take(4)
    own = take(packs - 1)
    full = take(packs)
    vec_rows, logsum = take(2)
    hidden_out, flat_out, second_out, hidden_two_out, inner_out, active_out = take(6)
    qkv_out, attended_out = take(2)
    weight, vec_full, spread, qkv, attended, attended_in = take(6)
    hidden, attended_flat, second, inner, active, inner_block = take(6)
    own.insert(1, inner_block)
    z_sems, p_sems, c_sems, v_sems, a_sems, b_sems = (take(2) for _ in range(6))
    local, load, a_local, b_local, o_sem, i_sem = take(6)
    rows_all, width = images.shape
    count, _, _, _, block = qkv.shape
    depth = own[0].shape[1]
    group = width // n_seq
    heads = group // HD
    at = Place(n_seq, n_fsdp, depth)
    n_z = at.n_z
    at.greet()

    def vec_copy(src, dst, sem, f):
        return at.copy(src, vec_full.at[dst], v_sems, sem, at.s, f)

    def z_copy(p, d, arriving):
        dst = full[p].at[at.block, at.rows(at.from_f[d] if arriving else at.f)]
        return at.copy(own[p].at[at.block], dst, z_sems, (p, d), at.s, at.to_f[d])

    def plane(p, d, k, arriving):
        for half, steps in enumerate(PLAN):
            bit, masks, slot = steps[k]
            rows = at.rows(at.from_f[d], half)
            for i, m in enumerate(masks):
                src = full[p].at[flip_mask(at.block, m), rows]
                dst = full[p].at[flip_mask(at.block, m ^ (1 << bit)), rows] if arriving else src
                yield at.copy(src, dst, p_sems, (p, d, half, slot + i), flip(at.s, bit), at.f)

    def core_copy(p, d, arriving):
        f = at.from_f[d]
        src = own[p] if d == 0 else full[p].at[:, at.rows(f)]
        dst = full[p].at[:, at.rows(f + 1 - 2 * at.core if arriving else f)]
        return at.copy(src, dst, c_sems, (p, d), at.s, at.other)

    at.start([vec_copy(vec, at.f, d, at.to_f[d]) for d in range(1, n_z)])
    at.start([vec_copy(vec, at.f, 0, at.other)])
    at.start([z_copy(0, d, False) for d in range(1, n_z)])
    ff_own = inner_own.shape[1] // n_fsdp

    def relayout(rows, _):
        values = inner_own[rows, :]
        for q in range(BLOCKS):
            size = min(depth, ff_own - q * depth)
            inner_block[q, rows, :] = pieces_to_columns(
                lambda f, q=q, size=size: values[
                    :, f * ff_own + q * depth : f * ff_own + q * depth + size
                ],
                n_fsdp,
                size,
                depth,
            )
        return 0

    row_loop(depth, relayout)
    at.start([z_copy(p, d, False) for p in range(1, packs) for d in range(1, n_z)])
    keep = [
        pltpu.make_async_copy(own[p], full[p].at[:, at.rows(at.f)], local.at[p])
        for p in range(packs)
    ] + [pltpu.make_async_copy(vec, vec_full.at[at.f], local.at[packs])]
    for copy in keep:
        copy.start()
    at.start([core_copy(p, 0, False) for p in range(packs)])
    for d in range(1, n_z):
        arrive([vec_copy(vec, at.from_f[d], d, at.to_f[d])])
        at.start([vec_copy(vec_full.at[at.from_f[d]], at.from_f[d], n_z - 1 + d, at.other)])
    for d in range(n_z):
        sem = n_z - 1 + d if d else 0
        f = at.from_f[d] + 1 - 2 * at.core
        arrive([vec_copy(vec_full.at[f], f, sem, at.other)])
    keep[packs].wait()

    vec_rows[...] = jnp.concatenate([wide(vec_full[f]) for f in range(n_fsdp)], axis=1)

    def first_norm(rows, _):
        normed, _ = normalize(wide(images[rows, :]))
        hidden[rows, :] = (normed * vec_rows[0:1, :] + vec_rows[1:2, :]).astype(LOW)
        return 0

    row_loop(rows_all, first_norm)

    def from_z(p, d):
        arrive([z_copy(p, d, True)])
        at.start(plane(p, d, 0, False))

    def second_step(p):
        for d in range(1, n_z):
            arrive(plane(p, d, 0, True))
            at.start(plane(p, d, 1, False))

    def to_core(p, d):
        arrive(plane(p, d, 1, True))
        at.start([core_copy(p, d, False)])

    def weight_load(w):
        return pltpu.make_async_copy(full[0].at[w], weight.at[w % 2], load.at[w % 2])

    send_heads = Exchange(at, spread, qkv, a_sems, a_local)
    send_tokens = Exchange(at, attended, attended_in, b_sems, b_local)

    for d in range(1, n_z):
        from_z(0, d)
    second_step(0)
    for d in range(1, n_z):
        from_z(1, d)
        to_core(0, d)
    for d in range(n_z):
        arrive([core_copy(0, d, True)])
    keep[0].wait()
    weight_load(0).start()
    for w in range(3):
        if w < 2:
            weight_load(w + 1).start()
        weight_load(w).wait()
        value = product(hidden[...], weight[w % 2])
        if w != 1:
            value = value + vec_rows[2 + w // 2 : 3 + w // 2, :]
        value = value.T.astype(LOW)
        for i in range(count):
            for t in range(n_seq):
                spread[i, t, w] = value[
                    t * group : (t + 1) * group, i * block : (i + 1) * block
                ]
    for i in range(count):
        send_heads.send(i)
    second_step(1)
    for d in range(1, n_z):
        from_z(2, d)
    for i in range(count):
        send_heads.receive(i)
        scatter_tokens(
            forward_heads(i, heads, n_seq, qkv.at[i], mask, logsum), n_seq, attended, i, 0
        )
        send_tokens.send(i)
        if i == 0:
            for d in range(1, n_z):
                to_core(1, d)
            second_step(2)
    saves = [
        pltpu.make_async_copy(qkv, qkv_out, o_sem.at[0]),
        pltpu.make_async_copy(attended, attended_out, o_sem.at[1]),
        pltpu.make_async_copy(hidden, hidden_out, o_sem.at[2]),
    ]
    for copy in saves:
        copy.start()

    def square_load(ref, q, slot):
        return pltpu.make_async_copy(ref.at[q], weight.at[slot], load.at[slot])

    square_load(full[0], 3, 0).start()
    keep[1].wait()
    for d in range(n_z):
        arrive([core_copy(1, d, True)])
    square_load(full[1], 0, 1).start()
    for i in range(count):
        send_tokens.receive(i)
        features = jnp.concatenate([attended_in[i, t, 0] for t in range(n_seq)], axis=0)
        attended_flat[i * block : (i + 1) * block, :] = wide(features).T.astype(LOW)

    square_load(full[0], 3, 0).wait()
    second[...] = product(attended_flat[...], weight[0])
    square_load(full[1], 1, 0).start()

    def second_norm(rows, _):
        value = wide(images[rows, :]) + second[rows, :] + vec_rows[4:5, :]
        second[rows, :] = value
        normed, _ = normalize(value)
        hidden[rows, :] = (normed * vec_rows[5:6, :] + vec_rows[6:7, :]).astype(LOW)
        return 0

    saves[2].wait()
    row_loop(rows_all, second_norm)
    more = [
        pltpu.make_async_copy(attended_flat, flat_out, o_sem.at[3]),
        pltpu.make_async_copy(second, second_out, o_sem.at[4]),
        pltpu.make_async_copy(hidden, hidden_two_out, o_sem.at[5]),
    ]
    for copy in more:
        copy.start()

    def inner_saves(q):
        slot = q % 2
        return [
            pltpu.make_async_copy(inner.at[slot], inner_out.at[q], i_sem.at[0, slot]),
            pltpu.make_async_copy(active.at[slot], active_out.at[q], i_sem.at[1, slot]),
        ]

    for q in range(BLOCKS):
        slot = q % 2
        if q >= 2:
            for copy in inner_saves(q - 2):
                copy.wait()
        square_load(full[1], q, 1 - slot).wait()
        inner[slot] = product(hidden[...], weight[1 - slot])
        if q + 2 < BLOCKS:
            square_load(full[1], q + 2, 1 - slot).start()

        def bend(rows, _, q=q, slot=slot):
            value = inner[slot, rows, :] + vec_rows[8 + q : 9 + q, :]
            inner[slot, rows, :] = value
            active[slot, rows, :] = gelu(value).astype(LOW)
            return 0

        row_loop(rows_all, bend)
        for copy in inner_saves(q):
            copy.start()
        if q + 1 < n_z:
            to_core(2, q + 1)
    for d in range(BLOCKS + 1, n_z):
        to_core(2, d)
    for q in (BLOCKS - 2, BLOCKS - 1):
        for copy in inner_saves(q):
            copy.wait()
    keep[2].wait()
    for d in range(n_z):
        arrive([core_copy(2, d, True)])
    for copy in saves[:2] + more:
        copy.wait()
    at.finish()


def spaces():
    return pl.BlockSpec(memory_space=pl.ANY), pl.BlockSpec(memory_space=pltpu.VMEM)


def pair(*dims):
    return [pltpu.SemaphoreType.DMA(dims), pltpu.SemaphoreType.DMA(dims)]


def forward_all(n_seq, n_fsdp, count, images, mask, vec, inner_weight, attn, outer):
    packs = 3
    rows, width = images.shape
    depth = width // n_fsdp
    length = mask.shape[1]
    n_z, group, block = n_fsdp // 2, width // n_seq, rows // count
    heads = group // HD
    dma, vmem, shape = pltpu.SemaphoreType.DMA, pltpu.VMEM, jax.ShapeDtypeStruct
    any_space, in_vmem = spaces()
    qkv = (count, n_seq, 3, group, block)
    att = (count, n_seq, 1, group, block)
    flat = (rows, width)
    return pl.pallas_call(
        functools.partial(forward_kernel, n_seq, n_fsdp, packs),
        out_shape=[shape((BLOCKS, width, width), LOW) for _ in range(packs)]
        + [
            shape((vec.shape[0], width), WIDE),
            shape((count, heads, length), WIDE),
            shape(flat, LOW),
            shape(flat, LOW),
            shape(flat, WIDE),
            shape(flat, LOW),
            shape((BLOCKS,) + flat, WIDE),
            shape((BLOCKS,) + flat, LOW),
            shape(qkv, LOW),
            shape(att, LOW),
        ],
        in_specs=[in_vmem] * 6,
        out_specs=[any_space] * packs + [in_vmem] * 2 + [any_space] * 8,
        scratch_shapes=[
            vmem((2, width, width), LOW),
            vmem((n_fsdp,) + vec.shape, LOW),
            vmem(qkv, LOW),
            vmem(qkv, LOW),
            vmem(att, LOW),
            vmem(att, LOW),
            vmem(flat, LOW),
            vmem(flat, LOW),
            vmem(flat, WIDE),
            vmem((2,) + flat, WIDE),
            vmem((2,) + flat, LOW),
            vmem((BLOCKS, depth, width), LOW),
            *pair(packs, n_z),
            *pair(packs, n_z, 2, BLOCKS - 1),
            *pair(packs, n_z),
            *pair(2 * n_z - 1),
            *pair(count, n_seq),
            *pair(count, n_seq),
            dma((packs + 1,)),
            dma((2,)),
            dma((count,)),
            dma((count,)),
            dma((6,)),
            dma((2, 2)),
        ],
        compiler_params=pltpu.CompilerParams(
            collective_id=0, has_side_effects=True, vmem_limit_bytes=VMEM_LIMIT
        ),
        name="forward_layer",
    )(images, mask, vec, inner_weight, attn, outer)


def add_rows(target, left, right, start, size):
    step = 16 if start % 16 == 0 and size % 16 == 0 else 8

    def body(i, _):
        rows = pl.ds(pl.multiple_of(start + i * step, step), step)
        target[rows, :] = (wide(left[rows, :]) + wide(right[rows, :])).astype(LOW)
        return 0

    lax.fori_loop(0, size // step, body, 0)


class Reduction:
    RING = 4
    Z_RING = 6

    @classmethod
    def scratch(cls, n_seq, n_fsdp, packs, depth, width):
        n_z, upper = n_fsdp // 2, n_seq.bit_length() - 3
        dma, vmem, ring = pltpu.SemaphoreType.DMA, pltpu.VMEM, cls.RING
        piece = (depth, width)
        return [
            vmem((ring, BLOCKS) + piece, LOW),
            vmem((ring, BLOCKS) + piece, LOW),
            vmem((ring, BLOCKS - 1) + piece, LOW),
            vmem((cls.Z_RING,) + piece, LOW),
            vmem((packs, n_z) + piece, LOW),
            vmem((packs, BLOCKS) + piece, LOW),
            vmem((max(upper, 1), ring, BLOCKS) + (piece if upper else (16, 128)), LOW),
            dma((ring,)),
            *pair(ring),
            *pair(ring, 2, BLOCKS - 1),
            *pair(packs, n_z),
            *pair(packs, 2, BLOCKS - 1),
            *pair(max(upper, 1), ring),
            pltpu.SemaphoreType.REGULAR((3 + max(upper, 1),)),
        ]

    def __init__(self, at, packs, grads, scratch):
        self.at, self.packs, self.grads = at, packs, grads
        (
            self.held,
            self.core_in,
            self.plane_in,
            self.z_out,
            self.z_in,
            self.total,
            self.upper_in,
            self.load_sem,
            *sems,
            self.credit,
        ) = scratch
        self.c_sems, self.p_sems, self.z_sems, self.g_sems, self.u_sems = (
            sems[2 * i : 2 * i + 2] for i in range(5)
        )
        self.upper = at.n_seq.bit_length() - 3
        self.count = packs * at.n_z
        self.flight = {}
        self.z_flight = []

    def where(self, i):
        p, t = divmod(i, self.at.n_z)
        return p, t, lax.rem(self.at.z + t + 1, self.at.n_z), i % self.RING

    def give(self, kind, s, f):
        pl.semaphore_signal(
            self.credit.at[kind], inc=1, device_id={"seq": s, "fsdp": f}, device_id_type=MESH
        )

    def need(self, i, kind):
        if i >= self.RING:
            pl.semaphore_wait(self.credit.at[kind], 1)

    def load(self, i):
        p, _, z, slot = self.where(i)
        rows = self.at.rows(2 * z + self.at.core)
        return pltpu.make_async_copy(
            self.grads[p].at[:, rows], self.held.at[slot], self.load_sem.at[slot]
        )

    def to_partner(self, i):
        p, _, z, slot = self.where(i)
        at = self.at
        rows = at.rows(2 * z + 1 - at.core)
        return at.copy(
            self.grads[p].at[:, rows], self.core_in.at[slot], self.c_sems, slot, at.s, at.other
        )

    def start(self, i):
        if i >= self.RING:
            for copy in self.flight.pop(i - self.RING):
                copy.wait_send()
        self.need(i, 0)
        self.flight[i] = []
        self.go(i, [self.to_partner(i)])
        self.load(i).start()

    def go(self, i, copies):
        for copy in copies:
            copy.start()
            self.flight[i].append(copy)

    def plane(self, i, k):
        at = self.at
        slot = i % self.RING
        for half, steps in enumerate(PLAN):
            bit, masks, first = steps[k]
            for j, m in enumerate(masks):
                src = self.held.at[slot, flip_mask(at.block, m ^ (1 << bit)), at.part(half)]
                dst = self.plane_in.at[slot, first + j, at.part(half)]
                yield at.copy(
                    src, dst, self.p_sems, (slot, half, first + j), flip(at.s, bit), at.f
                )

    def z_copy(self, i, number=0):
        p, t, z, _ = self.where(i)
        at = self.at
        return at.copy(
            self.z_out.at[number % self.Z_RING],
            self.z_in.at[p, t],
            self.z_sems,
            (p, t),
            at.s,
            2 * z + at.core,
        )

    def spread(self, p, k, arriving):
        at = self.at
        for half, steps in enumerate(PLAN):
            bit, masks, slot = steps[k]
            for i, m in enumerate(masks):
                src = self.total.at[p, flip_mask(at.block, m), at.part(half)]
                dst = self.total.at[p, flip_mask(at.block, m ^ (1 << bit)), at.part(half)]
                yield at.copy(
                    src,
                    dst if arriving else src,
                    self.g_sems,
                    (p, half, slot + i),
                    flip(at.s, bit),
                    at.f,
                )

    def add_all(self, slot, term):
        def body(q, _):
            held = self.held.at[slot, q]
            add_rows(held, held, term.at[q], 0, self.at.depth)
            return 0

        lax.fori_loop(0, BLOCKS, body, 0)

    def stage_core(self, i):
        at = self.at
        slot = i % self.RING
        more = i + self.RING < self.count
        self.load(i).wait()
        arrive([self.to_partner(i)])
        self.add_all(slot, self.core_in.at[slot])
        if more:
            self.give(0, at.s, at.other)
        for u in range(self.upper):
            peer = flip(at.s, 2 + u)
            self.need(i, 3 + u)
            copy = at.copy(
                self.held.at[slot], self.upper_in.at[u, slot], self.u_sems, (u, slot), peer, at.f
            )
            copy.start()
            copy.wait()
            self.add_all(slot, self.upper_in.at[u, slot])
            if more:
                self.give(3 + u, peer, at.f)
        self.need(i, 1)
        self.need(i, 2)
        self.go(i, self.plane(i, 1))

    def stage_plane(self, i, k):
        at = self.at
        p, t, _, slot = self.where(i)
        last = t == at.n_z - 1
        arrive(self.plane(i, k))
        number = len(self.z_flight)
        if k == 0 and not last and number >= self.Z_RING:
            self.z_flight[number - self.Z_RING].wait_send()
        for half, steps in enumerate(PLAN):
            _, masks, first = steps[k]
            for j, m in enumerate(masks):
                held = self.held.at[slot, flip_mask(at.block, m)]
                target = held
                if k == 0:
                    target = self.z_in.at[p, t] if last else self.z_out.at[number % self.Z_RING]
                add_rows(target, held, self.plane_in.at[slot, first + j], *at.halves[half])
        if k > 0:
            self.go(i, self.plane(i, k - 1))
            return
        if i + self.RING < self.count:
            for bit in range(2):
                self.give(1 + bit, flip(at.s, bit), at.f)
        if not last:
            copy = self.z_copy(i, number)
            copy.start()
            self.z_flight.append(copy)

    def stage_total(self, p):
        at = self.at
        last = at.n_z - 1
        arrive(self.z_copy(p * at.n_z + t) for t in range(last))

        def body(rows, _):
            value = wide(self.z_in[p, last, rows, :])
            for t in range(last):
                value = value + wide(self.z_in[p, t, rows, :])
            self.total[p, at.block, rows, :] = value.astype(LOW)
            return 0

        row_loop(at.depth, body)
        at.start(self.spread(p, 0, False))

    def stage_spread(self, p, k):
        arrive(self.spread(p, k - 1, True))
        if k < 2:
            self.at.start(self.spread(p, k, False))

    def events(self, i, time):
        return [
            (time, 0, functools.partial(self.stage_core, i)),
            (time + 1, 1, functools.partial(self.stage_plane, i, 1)),
            (time + 2, 2, functools.partial(self.stage_plane, i, 0)),
        ]

    def finish(self):
        for copies in self.flight.values():
            for copy in copies:
                copy.wait_send()
        for copy in self.z_flight[-self.Z_RING :]:
            copy.wait_send()


def backward_kernel(n_seq, n_fsdp, ff_own, *refs):
    refs = list(refs)

    def take(n):
        items = refs[:n]
        del refs[:n]
        return items

    packs = 3
    w_attn, w_inner, w_outer = take(3)
    inner_in, active_in, second_in, hidden_two_in, flat_in, hidden_one_in = take(6)
    images_in, cot_in, qkv_in, attended_in, mask, logsum, vecs = take(7)
    layer_out, images_grad, out_outer, out_attn, inner_grad, vec_out = take(6)
    grads = take(packs)
    square, op_one, op_two, act, low, inner, tmp, gs, back = take(9)
    qkv, attended, grad_spread, grad_heads, back_spread, back_in = take(6)
    vec_acc, sums, v_work, v_came, v_z = take(5)
    a_sems, b_sems, v_sems = take(2), take(2), take(2)
    a_local, b_local, s_sem, o_sem, act_sem, g_sem, h_sem, f_sem = take(8)
    rows_all, width = op_one.shape
    count, _, _, group, block = back_in.shape
    heads = group // HD
    depth = width // n_fsdp
    at = Place(n_seq, n_fsdp, depth)
    n_z, bits = at.n_z, n_seq.bit_length() - 1
    red = Reduction(at, packs, grads, refs)
    chunk = lambda p, t: p * n_z + t

    class Load:
        def __init__(self, target, sem):
            self.target, self.sem, self.copy = target, sem, None

        def start(self, src):
            self.copy = pltpu.make_async_copy(src, self.target, self.sem)
            self.copy.start()

        def wait(self):
            self.copy.wait()

    squares = [Load(square.at[k], s_sem.at[k]) for k in range(3)]
    ops = [Load(op_one, o_sem.at[0]), Load(op_two, o_sem.at[1])]
    acts = [Load(act.at[k], act_sem.at[k]) for k in range(2)]
    inners = Load(inner, f_sem.at[0])
    heads_in = [Load(qkv, h_sem.at[0]), Load(attended, h_sem.at[1])]
    stores = {}

    def store(key, src, dst, sem):
        stores[key] = pltpu.make_async_copy(src, dst, sem)
        stores[key].start()

    def stored(*keys):
        for key in keys:
            stores.pop(key).wait()

    send_heads = Exchange(at, grad_spread, grad_heads, a_sems, a_local)
    send_tokens = Exchange(at, back_spread, back_in, b_sems, b_local)

    ops[0].start(cot_in)
    acts[0].start(active_in.at[0])
    acts[1].start(active_in.at[1])
    ops[1].start(hidden_two_in)
    squares[2].start(w_outer.at[0])
    inners.start(inner_in.at[0])
    at.greet()
    ops[0].wait()

    for q in range(BLOCKS):
        acts[q % 2].wait()
        if q >= 2:
            stored(("outer", q - 2))
        tall_product(act.at[q % 2], op_one, square.at[q % 2])
        store(("outer", q), square.at[q % 2], grads[0].at[q], g_sem.at[0, q])
        if q + 2 < BLOCKS:
            acts[q % 2].start(active_in.at[q + 2])
    stored(("outer", BLOCKS - 2))
    squares[0].start(w_inner.at[0])
    stored(("outer", BLOCKS - 1))
    ops[1].wait()

    def mlp(q):
        more = q + 1 < BLOCKS
        squares[2].wait()
        tmp[...] = product_back(op_one[...], square[2])
        if more:
            squares[2].start(w_outer.at[q + 1])
        else:
            squares[2].start(w_attn.at[3])
        inners.wait()
        sums[0] = jnp.zeros_like(sums[0])

        def body(rows, _):
            value = tmp[rows, :] * gelu_slope(inner[rows, :])
            sums[0] += fold(value)
            low[rows, :] = value.astype(LOW)
            return 0

        row_loop(rows_all, body)
        vec_acc[8 + q : 9 + q, :] = column_sum(sums[0])
        inners.start(inner_in.at[q + 1] if more else second_in)
        squares[0].wait()
        if q == 0:
            gs[...] = product_back(low[...], square[0])
        else:
            gs[...] += product_back(low[...], square[0])
        if more:
            squares[0].start(w_inner.at[q + 1])
        if q > 0:
            stored(("inner", q - 1))
        tall_product(op_two, low, square.at[1])
        store(("inner", q), square.at[1], grads[1].at[q], g_sem.at[1, q])
        if not more:
            ops[1].start(flat_in)

    def second_norm():
        inners.wait()
        for k in range(4):
            sums[k] = jnp.zeros_like(sums[k])

        def body(rows, _):
            normed, factor = normalize(inner[rows, :])
            grad = gs[rows, :]
            up = wide(op_one[rows, :])
            value = up + norm_back(grad * vecs[5:6, :], normed, factor)
            gs[rows, :] = value
            low[rows, :] = value.astype(LOW)
            sums[0] += fold(grad * normed)
            sums[1] += fold(grad)
            sums[2] += fold(value)
            sums[3] += fold(up)
            return 0

        row_loop(rows_all, body)
        for k, row in enumerate((5, 6, 4, 7)):
            vec_acc[row : row + 1, :] = column_sum(sums[k])

    def attended_grad():
        squares[2].wait()
        tmp[...] = product_back(low[...], square[2])
        for i in range(count):
            value = tmp[i * block : (i + 1) * block, :].T.astype(LOW)
            for t in range(n_seq):
                grad_spread[i, t, 0] = value[t * group : (t + 1) * group]
            send_heads.send(i)
        heads_in[0].start(qkv_in.at[0])
        heads_in[1].start(attended_in.at[0])
        stored(("inner", BLOCKS - 1))

    def out_grad():
        ops[1].wait()
        tall_product(op_two, low, square.at[1])
        store(("attn", 3), square.at[1], grads[2].at[3], g_sem.at[2, 3])
        ops[1].start(hidden_one_in)

    def image(i):
        send_heads.receive(i)
        for copy in heads_in:
            copy.wait()
        for w, value in enumerate(
            backward_heads(i, heads, n_seq, qkv, attended, grad_heads.at[i], mask, logsum)
        ):
            scatter_tokens(value, n_seq, back_spread, i, w)
        send_tokens.send(i)
        if i + 1 < count:
            heads_in[0].start(qkv_in.at[i + 1])
            heads_in[1].start(attended_in.at[i + 1])

    def collect(i):
        send_tokens.receive(i)
        for w in range(3):
            features = jnp.concatenate([back_in[i, t, w] for t in range(n_seq)], axis=0)
            back[w, i * block : (i + 1) * block, :] = wide(features).T.astype(LOW)

    def attn_grads():
        ops[1].wait()
        for w in range(3):
            slot = (0, 2, 1)[w]
            if slot == 1:
                stored(("attn", 3))
            tall_product(op_two, back.at[w], square.at[slot])
            store(("attn", w), square.at[slot], grads[2].at[w], g_sem.at[2, w])
        acts[0].start(images_in)
        for w in range(3):
            stored(("attn", w))
            slot = (0, 2, 1)[w]
            squares[slot].start(w_attn.at[w])

    def input_grad():
        for w in range(3):
            slot = (0, 2, 1)[w]
            squares[slot].wait()
            value = product_back(back[w], square[slot])
            if w == 0:
                tmp[...] = value
            else:
                tmp[...] += value
            squares[slot].start(w_outer.at[w])
        acts[0].wait()
        for k in range(4):
            sums[k] = jnp.zeros_like(sums[k])

        def body(rows, _):
            normed, factor = normalize(wide(act[0, rows, :]))
            grad = tmp[rows, :]
            gs[rows, :] += norm_back(grad * vecs[0:1, :], normed, factor)
            sums[0] += fold(grad * normed)
            sums[1] += fold(grad)
            sums[2] += fold(wide(back[0, rows, :]))
            sums[3] += fold(wide(back[2, rows, :]))
            return 0

        row_loop(rows_all, body)
        for k in range(4):
            vec_acc[k : k + 1, :] = column_sum(sums[k])
        store("images", gs, images_grad, f_sem.at[1])
        at.start([vec_copy(0)])
        acts[0].start(active_in.at[0])
        acts[1].start(active_in.at[1])

    def output():
        for q in range(BLOCKS):
            slot = (0, 2, 1, 0)[q]
            squares[slot].wait()
            acts[q % 2].wait()
            inner[...] += product(act[q % 2], square[slot])
            if q == 0:
                squares[0].start(w_outer.at[BLOCKS - 1])
            if q + 2 < BLOCKS:
                acts[q % 2].start(active_in.at[q + 2])

        def body(rows, _):
            inner[rows, :] += vecs[7:8, :]
            return 0

        row_loop(rows_all, body)
        store("layer", inner, layer_out, f_sem.at[2])

    def vec_copy(i):
        src = vec_acc if i == 0 else v_work.at[i - 1]
        peer = (at.s, at.other) if i == 0 else (flip(at.s, i - 1), at.f)
        return at.copy(src, v_came.at[i], v_sems, i, *peer)

    def vec_z(d, arriving):
        z = lax.div(at.from_f[d], 2) if arriving else at.z
        return at.copy(v_work.at[bits], v_z.at[z], v_sems, bits + d, at.s, at.to_f[d])

    def vec_stage(i):
        arrive([vec_copy(i)])
        v_work[i] = (vec_acc[...] if i == 0 else v_work[i - 1]) + v_came[i]
        if i < bits:
            at.start([vec_copy(i + 1)])
        else:
            at.start([vec_z(d, False) for d in range(1, n_z)])

    def vec_last():
        arrive([vec_z(d, True) for d in range(1, n_z)])
        value = v_work[bits]
        for d in range(1, n_z):
            value = value + v_z[lax.div(at.from_f[d], 2)]
        for f in range(n_fsdp):

            @pl.when(at.f == f)
            def _(f=f):
                vec_out[...] = value[:, f * depth : (f + 1) * depth]

    def relayout():
        def body(rows, _):
            parts = []
            for f in range(n_fsdp):
                for q in range(BLOCKS):
                    size = min(depth, ff_own - q * depth)
                    parts.append((q, f * depth, size))
            values = [red.total[1, q, rows, :] for q in range(BLOCKS)]
            inner_grad[rows, :] = jnp.concatenate(
                [values[q][:, first : first + size] for q, first, size in parts], axis=1
            )
            return 0

        row_loop(depth, body)

    def save(p, out):
        store(("out", p), red.total.at[p], out, g_sem.at[p, BLOCKS])

    events = []

    def add(time, call, *args):
        events.append((time, 10, functools.partial(call, *args)))

    gap = 2.5
    first_attn = 2 * n_z + gap
    for i in range(2 * n_z):
        events += red.events(i, i)
        add(-1 if i < red.RING else i - 1.4 if i < n_z else max(i - 1.4, n_z - 0.3), red.start, i)
    for t in range(n_z):
        events += red.events(chunk(2, t), first_attn + t)
        add(first_attn - 0.3 if t < red.RING else first_attn + t - 1.4, red.start, chunk(2, t))
    for q in range(BLOCKS):
        add(q * n_z / BLOCKS * 0.9 + 0.5, mlp, q)
    add(n_z - 0.4, second_norm)
    add(n_z - 0.35, attended_grad)
    add(n_z + 0.5, out_grad)
    for i in range(count):
        add(n_z + 1.5 + i, image, i)
        add(max(n_z + 3.5 + i, first_attn - 1.4 + 0.1 * i), collect, i)
    add(first_attn - 0.4, attn_grads)
    add(first_attn + 0.5, input_grad)
    for i in range(bits + 1):
        add(first_attn + 1.2 + i, vec_stage, i)
    add(first_attn + bits + 2.5, vec_last)
    add(first_attn + 1.5, output)
    for p, last in enumerate((n_z + 1, 2 * n_z + 1, first_attn + n_z + 1)):
        add(last + 1.1, red.stage_total, p)
        add(last + 1.8, red.stage_spread, p, 1)
        add(last + 2.6, red.stage_spread, p, 2)
    add(n_z + 3.7, save, 0, out_outer)
    add(2 * n_z + 3.7, relayout)
    add(first_attn + n_z + 3.7, save, 2, out_attn)
    run_events(events)
    stored(*list(stores))
    red.finish()
    at.finish()


def run_events(events):
    for _, _, call in sorted(events, key=lambda e: e[:2]):
        call()


def backward_all(n_seq, n_fsdp, ff_own, weights, saved, images, cot, mask, logsum, vecs):
    inner, active, second, hidden_two, flat, hidden_one, qkv, attended = saved
    rows, width = images.shape
    depth, n_z, bits = width // n_fsdp, n_fsdp // 2, n_seq.bit_length() - 1
    count = qkv.shape[0]
    any_space, in_vmem = spaces()
    dma, vmem, shape = pltpu.SemaphoreType.DMA, pltpu.VMEM, jax.ShapeDtypeStruct
    tokens = (rows, width)
    square = (BLOCKS, width, width)
    return pl.pallas_call(
        functools.partial(backward_kernel, n_seq, n_fsdp, ff_own),
        out_shape=[
            shape(tokens, WIDE),
            shape(tokens, WIDE),
            shape((BLOCKS, depth, width), LOW),
            shape((BLOCKS, depth, width), LOW),
            shape((depth, n_fsdp * ff_own), LOW),
            shape((vecs.shape[0], depth), WIDE),
        ]
        + [shape(square, LOW) for _ in range(3)],
        in_specs=[any_space] * 13 + [in_vmem] * 3,
        out_specs=[any_space] * 4 + [in_vmem] * 2 + [any_space] * 3,
        scratch_shapes=[
            vmem((3, width, width), LOW),
            vmem(tokens, LOW),
            vmem(tokens, LOW),
            vmem((2,) + tokens, LOW),
            vmem(tokens, LOW),
            vmem(tokens, WIDE),
            vmem(tokens, WIDE),
            vmem(tokens, WIDE),
            vmem((3,) + tokens, LOW),
            vmem(qkv.shape[1:], LOW),
            vmem(attended.shape[1:], LOW),
            vmem(attended.shape, LOW),
            vmem(attended.shape, LOW),
            vmem(qkv.shape, LOW),
            vmem(qkv.shape, LOW),
            vmem(vecs.shape, WIDE),
            vmem((4, 8, width), WIDE),
            vmem((bits + 1,) + vecs.shape, WIDE),
            vmem((bits + 1,) + vecs.shape, WIDE),
            vmem((n_z,) + vecs.shape, WIDE),
            *pair(count, n_seq),
            *pair(count, n_seq),
            *pair(bits + n_z),
            dma((count,)),
            dma((count,)),
            dma((3,)),
            dma((2,)),
            dma((2,)),
            dma((3, BLOCKS + 1)),
            dma((2,)),
            dma((3,)),
            *Reduction.scratch(n_seq, n_fsdp, 3, depth, width),
        ],
        compiler_params=pltpu.CompilerParams(
            collective_id=1, has_side_effects=True, vmem_limit_bytes=VMEM_LIMIT
        ),
        name="backward_layer",
    )(
        *weights,
        inner,
        active,
        second,
        hidden_two,
        flat,
        hidden_one,
        images,
        cot,
        qkv,
        attended,
        mask,
        logsum,
        vecs,
    )


def shards(
    n_seq,
    n_fsdp,
    images,
    key_mask,
    attn_gain,
    attn_shift,
    query_weight,
    key_weight,
    value_weight,
    query_bias,
    value_bias,
    out_weight,
    out_bias,
    mlp_gain,
    mlp_shift,
    inner_weight,
    inner_bias,
    outer_weight,
    outer_bias,
    cotangent,
):
    count, block, width = images.shape
    rows = count * block
    depth = query_weight.shape[0]
    ff_own = outer_weight.shape[0]
    slack = BLOCKS * depth - ff_own
    small = [
        attn_gain,
        attn_shift,
        query_bias,
        value_bias,
        out_bias,
        mlp_gain,
        mlp_shift,
        outer_bias,
        jnp.pad(inner_bias, (0, slack + BLOCKS * depth)),
    ]
    vec = jnp.concatenate(small).reshape(16, depth)
    mask = jnp.where(key_mask > 0, 0.0, MASKED).astype(WIDE)[:, :, None]
    tokens = images.reshape(rows, width)
    forward = forward_all(
        n_seq,
        n_fsdp,
        count,
        tokens,
        mask,
        vec,
        inner_weight,
        jnp.stack((query_weight, key_weight, value_weight, out_weight)),
        jnp.pad(outer_weight, ((0, slack), (0, 0))).reshape(BLOCKS, depth, width),
    )
    weights, vecs, logsum = forward[:3], forward[3], forward[4]
    hidden_one, flat, second, hidden_two, inner, active, qkv, attended = forward[5:]
    layer_out, images_grad, outer_sum, attn_sum, inner_grad, vec_sum = backward_all(
        n_seq,
        n_fsdp,
        ff_own,
        weights,
        (inner, active, second, hidden_two, flat, hidden_one, qkv, attended),
        tokens,
        cotangent.reshape(rows, width),
        mask,
        logsum,
        vecs,
    )[:6]
    attn = wide(attn_sum)
    return (
        layer_out.reshape(count, block, width),
        images_grad.reshape(count, block, width),
        vec_sum[0],
        vec_sum[1],
        attn[0],
        attn[1],
        attn[2],
        vec_sum[2],
        vec_sum[3],
        attn[3],
        vec_sum[4],
        vec_sum[5],
        vec_sum[6],
        wide(inner_grad),
        vec_sum[8 : 8 + BLOCKS].reshape(BLOCKS * depth)[:ff_own],
        wide(outer_sum.reshape(BLOCKS * depth, width)[:ff_own]),
        vec_sum[7],
    )


def solution(mesh):
    vector, matrix, tokens = P("fsdp"), P("fsdp", None), P("fsdp", "seq", None)
    params = (
        vector,
        vector,
        matrix,
        matrix,
        matrix,
        vector,
        vector,
        matrix,
        vector,
        vector,
        vector,
        matrix,
        vector,
        matrix,
        vector,
    )
    return jax.shard_map(
        functools.partial(shards, mesh.shape["seq"], mesh.shape["fsdp"]),
        mesh=mesh,
        in_specs=(tokens, matrix) + params + (tokens,),
        out_specs=(tokens, tokens) + params,
        check_vma=False,
    )
```

```python
import functools

import jax
import jax.numpy as jnp
from jax import lax
from jax.experimental import pallas as pl
from jax.experimental.pallas import tpu as pltpu
from jax.sharding import PartitionSpec as P

HD = 72
EPSILON = 1e-06
MASKED = -1e30
LOG2_E = 1.4426950408889634
MESH = pl.DeviceIdType.MESH
VMEM_LIMIT = 67_000_000
BLOCKS = 4
LOW = jnp.bfloat16
WIDE = jnp.float32


def wide(values):
    return values.astype(WIDE)


def product(left, right):
    return jnp.dot(left, right, preferred_element_type=WIDE)


def product_rows(left, right):
    return lax.dot_general(left, right, (((0,), (0,)), ((), ())), preferred_element_type=WIDE)


def product_back(left, right):
    return lax.dot_general(left, right, (((1,), (1,)), ((), ())), preferred_element_type=WIDE)


def flip(index, bit):
    on = lax.rem(lax.div(index, 1 << bit), 2)
    return index + (1 - 2 * on) * (1 << bit)


def flip_mask(index, mask):
    bit = 0
    while mask >> bit:
        if (mask >> bit) & 1:
            index = flip(index, bit)
        bit += 1
    return index


PLAN = (((0, (0,), 0), (1, (0, 1), 1)), ((1, (0,), 0), (0, (0, 2), 1)))


class Place:
    def __init__(self, n_seq, n_fsdp, depth):
        self.n_seq, self.n_fsdp, self.depth = n_seq, n_fsdp, depth
        self.n_z = n_fsdp // 2
        self.s, self.f = lax.axis_index("seq"), lax.axis_index("fsdp")
        self.core, self.z = lax.rem(self.f, 2), lax.div(self.f, 2)
        self.block = lax.rem(self.s, BLOCKS)
        self.other = self.f + 1 - 2 * self.core
        n_z = self.n_z
        self.across = [flip_mask(self.z, d) for d in range(n_z)]
        self.to_f = self.from_f = [z * 2 + self.core for z in self.across]
        self.to_s = self.from_s = [flip_mask(self.s, d) for d in range(n_seq)]
        first = depth // 32 * 16
        self.halves = ((0, first), (first, depth - first))
        self.sent = []

    def greet(self):
        barrier = pltpu.get_barrier_semaphore()
        peers = [(self.s, self.other)]
        peers += [(self.s, f) for f in self.to_f[1:]]
        peers += [(s, self.f) for s in self.to_s[1:]]
        for s, f in peers:
            pl.semaphore_signal(
                barrier, inc=1, device_id={"seq": s, "fsdp": f}, device_id_type=MESH
            )
        pl.semaphore_wait(barrier, len(peers))

    def copy(self, src, dst, sems, index, s, f):
        return pltpu.make_async_remote_copy(
            src_ref=src,
            dst_ref=dst,
            send_sem=sems[0].at[index],
            recv_sem=sems[1].at[index],
            device_id={"seq": s, "fsdp": f},
            device_id_type=MESH,
        )

    def start(self, copies):
        for copy in copies:
            copy.start()
            self.sent.append(copy)

    def finish(self):
        for copy in self.sent:
            copy.wait_send()

    def rows(self, f, half=None):
        offset, size = (0, self.depth) if half is None else self.halves[half]
        return pl.ds(pl.multiple_of(f * self.depth + offset, 8), size)

    def part(self, half):
        return pl.ds(*self.halves[half])


def arrive(copies):
    for copy in copies:
        copy.wait_recv()


class Exchange:
    def __init__(self, place, out, into, sems, local):
        self.place, self.out, self.into, self.sems, self.local = place, out, into, sems, local

    def send(self, i):
        at = self.place
        at.start(
            at.copy(
                self.out.at[i, at.to_s[d]],
                self.into.at[i, at.s],
                self.sems,
                (i, d),
                at.to_s[d],
                at.f,
            )
            for d in range(1, at.n_seq)
        )
        self.keep(i).start()

    def keep(self, i):
        at = self.place
        return pltpu.make_async_copy(
            self.out.at[i, at.s], self.into.at[i, at.s], self.local.at[i]
        )

    def receive(self, i):
        at = self.place
        arrive(
            at.copy(
                self.out.at[i, at.to_s[d]],
                self.into.at[i, at.from_s[d]],
                self.sems,
                (i, d),
                at.to_s[d],
                at.f,
            )
            for d in range(1, at.n_seq)
        )
        self.keep(i).wait()


def heads_of(ref, w, head, n_seq):
    rows = slice(head * HD, (head + 1) * HD)
    return jnp.concatenate([ref[t, w, rows, :] for t in range(n_seq)], axis=1)


def normalize(values):
    center = values - jnp.mean(values, axis=-1, keepdims=True)
    factor = lax.rsqrt(jnp.mean(center * center, axis=-1, keepdims=True) + EPSILON)
    return (center * factor, factor)


def norm_back(grad_normed, normed, factor):
    first = jnp.mean(grad_normed, axis=-1, keepdims=True)
    second = jnp.mean(grad_normed * normed, axis=-1, keepdims=True)
    return factor * (grad_normed - first - normed * second)


GELU_SCALE = 0.7978845608028654
GELU_CUBE = 0.044715


def gelu(u):
    return 0.5 * u * (1.0 + jnp.tanh(GELU_SCALE * (u + GELU_CUBE * (u * u * u))))


def gelu_slope(u):
    square = u * u
    bent = jnp.tanh(GELU_SCALE * (u + GELU_CUBE * (u * square)))
    inner = GELU_SCALE * (1.0 + 3.0 * GELU_CUBE * square)
    return 0.5 * (1.0 + bent) + 0.5 * u * (1.0 - bent * bent) * inner


def row_loop(count, body, carry=0, step=16):
    step = step if count % step == 0 else 8
    return lax.fori_loop(
        0,
        count // step,
        lambda i, kept: body(pl.ds(pl.multiple_of(i * step, step), step), kept),
        carry,
    )


def fold(values):
    return sum(values[8 * i : 8 * i + 8] for i in range(values.shape[0] // 8))


def column_sum(kept):
    return jnp.sum(kept, axis=0, keepdims=True)


def tall_product(left, right, out):
    width = left.shape[1]
    tile = 384 if width % 384 == 0 else width

    def body(i, _):
        cols = pl.ds(pl.multiple_of(i * tile, 128), tile)
        out[cols, :] = product_rows(left[:, cols], right[...]).astype(LOW)
        return 0

    lax.fori_loop(0, width // tile, body, 0)


def pieces_to_columns(read, n_fsdp, size, width):
    parts = []
    for f in range(n_fsdp):
        piece = read(f)
        if size < width:
            piece = jnp.concatenate(
                [piece, jnp.zeros((piece.shape[0], width - size), piece.dtype)], axis=1
            )
        parts.append(piece)
    return jnp.concatenate(parts, axis=1)


def forward_heads(i, heads, n_seq, qkv, mask, logsum):
    scale = HD ** (-0.5) * LOG2_E
    outs, sums = [], []
    for h in range(heads):
        query, keys, values = (heads_of(qkv, w, h, n_seq) for w in range(3))
        scores = product_rows(keys, query) + mask[i]
        highest = jnp.max(scores, axis=0, keepdims=True)
        weights = jnp.exp2((scores - highest) * scale)
        total = jnp.sum(weights, axis=0, keepdims=True)
        outs.append(product(values, (weights * (1.0 / total)).astype(LOW)))
        sums.append(highest * scale + jnp.log2(total))
    logsum[i] = jnp.concatenate(sums, axis=0)
    return jnp.concatenate(outs, axis=0)


def backward_heads(i, heads, n_seq, qkv, attended, grad, mask, logsum):
    scale = HD ** (-0.5)
    grads = [[], [], []]
    for h in range(heads):
        query, keys, values = (heads_of(qkv, w, h, n_seq) for w in range(3))
        grad_out = heads_of(grad, 0, h, n_seq)
        delta = jnp.sum(
            wide(grad_out) * wide(heads_of(attended, 0, h, n_seq)), axis=0, keepdims=True
        )
        scores = product_rows(keys, query) * (scale * LOG2_E)
        chance = jnp.exp2(scores + mask[i] - logsum[i, h : h + 1, :])
        grad_scores = chance * (product_rows(values, grad_out) - delta) * scale
        grads[2].append(product_back(grad_out, chance.astype(LOW)))
        grad_scores = grad_scores.astype(LOW)
        grads[0].append(product(keys, grad_scores))
        grads[1].append(product_back(query, grad_scores))
    return [jnp.concatenate(item, axis=0) for item in grads]


def scatter_tokens(value, n_seq, out, i, w):
    block = value.shape[1] // n_seq
    low = value.astype(LOW)
    for t in range(n_seq):
        out[i, t, w] = low[:, t * block : (t + 1) * block]


def forward_kernel(n_seq, n_fsdp, packs, *refs):
    refs = list(refs)

    def take(n):
        items = refs[:n]
        del refs[:n]
        return items

    images, mask, vec, inner_own, cot = take(5)
    own = take(packs - 1)
    full = take(packs)
    vec_rows, logsum = take(2)
    hidden_out, flat_out, second_out, hidden_two_out, inner_out, active_out, grad_out = take(7)
    qkv_out, attended_out = take(2)
    weight, vec_full, spread, qkv, attended, attended_in = take(6)
    hidden, attended_flat, second, inner, active, inner_block, stage = take(7)
    own.insert(1, inner_block)
    z_sems, p_sems, c_sems, v_sems, a_sems, b_sems = (take(2) for _ in range(6))
    local, load, a_local, b_local, o_sem, i_sem = take(6)
    rows_all, width = images.shape
    count, _, _, _, block = qkv.shape
    depth = own[0].shape[1]
    group = width // n_seq
    heads = group // HD
    at = Place(n_seq, n_fsdp, depth)
    n_z = at.n_z
    at.greet()

    def vec_copy(src, dst, sem, f):
        return at.copy(src, vec_full.at[dst], v_sems, sem, at.s, f)

    def z_copy(p, d, arriving):
        dst = full[p].at[at.block, at.rows(at.from_f[d] if arriving else at.f)]
        return at.copy(own[p].at[at.block], dst, z_sems, (p, d), at.s, at.to_f[d])

    def plane(p, d, k, arriving):
        for half, steps in enumerate(PLAN):
            bit, masks, slot = steps[k]
            rows = at.rows(at.from_f[d], half)
            for i, m in enumerate(masks):
                src = full[p].at[flip_mask(at.block, m), rows]
                dst = full[p].at[flip_mask(at.block, m ^ (1 << bit)), rows] if arriving else src
                yield at.copy(src, dst, p_sems, (p, d, half, slot + i), flip(at.s, bit), at.f)

    def core_copy(p, d, arriving):
        f = at.from_f[d]
        src = own[p] if d == 0 else full[p].at[:, at.rows(f)]
        dst = full[p].at[:, at.rows(f + 1 - 2 * at.core if arriving else f)]
        return at.copy(src, dst, c_sems, (p, d), at.s, at.other)

    at.start([vec_copy(vec, at.f, d, at.to_f[d]) for d in range(1, n_z)])
    at.start([vec_copy(vec, at.f, 0, at.other)])
    at.start([z_copy(0, d, False) for d in range(1, n_z)])
    ff_own = inner_own.shape[1] // n_fsdp

    def relayout(rows, _):
        values = inner_own[rows, :]
        for q in range(BLOCKS):
            size = min(depth, ff_own - q * depth)
            inner_block[q, rows, :] = pieces_to_columns(
                lambda f, q=q, size=size: values[
                    :, f * ff_own + q * depth : f * ff_own + q * depth + size
                ],
                n_fsdp,
                size,
                depth,
            )
        return 0

    row_loop(depth, relayout)
    at.start([z_copy(p, d, False) for p in range(1, packs) for d in range(1, n_z)])
    keep = [
        pltpu.make_async_copy(own[p], full[p].at[:, at.rows(at.f)], local.at[p])
        for p in range(packs)
    ] + [pltpu.make_async_copy(vec, vec_full.at[at.f], local.at[packs])]
    for copy in keep:
        copy.start()
    at.start([core_copy(p, 0, False) for p in range(packs)])
    for d in range(1, n_z):
        arrive([vec_copy(vec, at.from_f[d], d, at.to_f[d])])
        at.start([vec_copy(vec_full.at[at.from_f[d]], at.from_f[d], n_z - 1 + d, at.other)])
    for d in range(n_z):
        sem = n_z - 1 + d if d else 0
        f = at.from_f[d] + 1 - 2 * at.core
        arrive([vec_copy(vec_full.at[f], f, sem, at.other)])
    keep[packs].wait()

    vec_rows[...] = jnp.concatenate([wide(vec_full[f]) for f in range(n_fsdp)], axis=1)

    def first_norm(rows, _):
        normed, _ = normalize(wide(images[rows, :]))
        hidden[rows, :] = (normed * vec_rows[0:1, :] + vec_rows[1:2, :]).astype(LOW)
        return 0

    row_loop(rows_all, first_norm)

    def from_z(p, d):
        arrive([z_copy(p, d, True)])
        at.start(plane(p, d, 0, False))

    def second_step(p, d):
        arrive(plane(p, d, 0, True))
        at.start(plane(p, d, 1, False))

    def to_core(p, d):
        arrive(plane(p, d, 1, True))
        at.start([core_copy(p, d, False)])

    def weight_load(w):
        return pltpu.make_async_copy(full[0].at[w], weight.at[w % 2], load.at[w % 2])

    send_heads = Exchange(at, spread, qkv, a_sems, a_local)
    send_tokens = Exchange(at, attended, attended_in, b_sems, b_local)

    def flow(p, shift):
        for k in range(n_z + 1):
            for late, step in enumerate((from_z, second_step, to_core)):
                if 0 <= k - late < n_z - 1:
                    yield k + shift, functools.partial(step, p, k - late + 1)

    for _, step in list(flow(0, 0))[:-1]:
        step()
    later = sorted(list(flow(1, 0)) + list(flow(2, 2.6)), key=lambda item: item[0])
    later = [step for _, step in later]
    later.pop(0)()
    to_core(0, n_z - 1)
    cuts = [len(later) * k // 17 for k in (0, 4, 7, 11, 14, 16, 17)]
    later = [later[a:b] for a, b in zip(cuts, cuts[1:])]

    def go_on():
        for step in later.pop(0) if later else ():
            step()

    for d in range(n_z):
        arrive([core_copy(0, d, True)])
    keep[0].wait()
    weight_load(0).start()
    for w in range(3):
        if w < 2:
            weight_load(w + 1).start()
        weight_load(w).wait()
        value = product(hidden[...], weight[w % 2])
        if w != 1:
            value = value + vec_rows[2 + w // 2 : 3 + w // 2, :]
        value = value.T.astype(LOW)
        for i in range(count):
            for t in range(n_seq):
                spread[i, t, w] = value[
                    t * group : (t + 1) * group, i * block : (i + 1) * block
                ]
    for i in range(count):
        send_heads.send(i)
    go_on()
    for i in range(count):
        send_heads.receive(i)
        scatter_tokens(
            forward_heads(i, heads, n_seq, qkv.at[i], mask, logsum), n_seq, attended, i, 0
        )
        send_tokens.send(i)
        go_on()
    saves = [
        pltpu.make_async_copy(qkv, qkv_out, o_sem.at[0]),
        pltpu.make_async_copy(attended, attended_out, o_sem.at[1]),
        pltpu.make_async_copy(hidden, hidden_out, o_sem.at[2]),
    ]
    for copy in saves:
        copy.start()

    def square_load(ref, q, slot):
        return pltpu.make_async_copy(ref.at[q], weight.at[slot], load.at[slot])

    square_load(full[0], 3, 0).start()
    keep[1].wait()
    for d in range(n_z):
        arrive([core_copy(1, d, True)])
    square_load(full[1], 0, 1).start()
    for i in range(count):
        send_tokens.receive(i)
        features = jnp.concatenate([attended_in[i, t, 0] for t in range(n_seq)], axis=0)
        attended_flat[i * block : (i + 1) * block, :] = wide(features).T.astype(LOW)

    square_load(full[0], 3, 0).wait()
    second[...] = product(attended_flat[...], weight[0])
    square_load(full[1], 1, 0).start()

    def second_norm(rows, _):
        value = wide(images[rows, :]) + second[rows, :] + vec_rows[4:5, :]
        second[rows, :] = value
        normed, _ = normalize(value)
        hidden[rows, :] = (normed * vec_rows[5:6, :] + vec_rows[6:7, :]).astype(LOW)
        return 0

    saves[2].wait()
    row_loop(rows_all, second_norm)
    more = [
        pltpu.make_async_copy(attended_flat, flat_out, o_sem.at[3]),
        pltpu.make_async_copy(second, second_out, o_sem.at[4]),
        pltpu.make_async_copy(hidden, hidden_two_out, o_sem.at[5]),
    ]
    for copy in more:
        copy.start()

    def inner_saves(q):
        slot = q % 2
        return [
            pltpu.make_async_copy(inner.at[slot], inner_out.at[q], i_sem.at[0, slot]),
            pltpu.make_async_copy(active.at[slot], active_out.at[q], i_sem.at[1, slot]),
            pltpu.make_async_copy(stage.at[slot], grad_out.at[q], i_sem.at[2, slot]),
        ]

    for q in range(BLOCKS):
        slot = q % 2
        if q >= 2:
            for copy in inner_saves(q - 2):
                copy.wait()
        square_load(full[1], q, 1 - slot).wait()
        inner[slot] = product(hidden[...], weight[1 - slot])
        if q + 2 < BLOCKS:
            square_load(full[1], q + 2, 1 - slot).start()

        def bend(rows, _, q=q, slot=slot):
            value = inner[slot, rows, :] + vec_rows[8 + q : 9 + q, :]
            inner[slot, rows, :] = value
            active[slot, rows, :] = gelu(value).astype(LOW)
            return 0

        row_loop(rows_all, bend)
        tall_product(active.at[slot], cot, stage.at[slot])
        for copy in inner_saves(q):
            copy.start()
        if q < BLOCKS - 1:
            go_on()
    for q in (BLOCKS - 2, BLOCKS - 1):
        for copy in inner_saves(q):
            copy.wait()
    keep[2].wait()
    for d in range(n_z):
        arrive([core_copy(2, d, True)])
    for copy in saves[:2] + more:
        copy.wait()
    at.finish()


def spaces():
    return pl.BlockSpec(memory_space=pl.ANY), pl.BlockSpec(memory_space=pltpu.VMEM)


def pair(*dims):
    return [pltpu.SemaphoreType.DMA(dims), pltpu.SemaphoreType.DMA(dims)]


def forward_all(n_seq, n_fsdp, count, images, mask, vec, inner_weight, cot, attn, outer):
    packs = 3
    rows, width = images.shape
    depth = width // n_fsdp
    length = mask.shape[1]
    n_z, group, block = n_fsdp // 2, width // n_seq, rows // count
    heads = group // HD
    dma, vmem, shape = pltpu.SemaphoreType.DMA, pltpu.VMEM, jax.ShapeDtypeStruct
    any_space, in_vmem = spaces()
    qkv = (count, n_seq, 3, group, block)
    att = (count, n_seq, 1, group, block)
    flat = (rows, width)
    return pl.pallas_call(
        functools.partial(forward_kernel, n_seq, n_fsdp, packs),
        out_shape=[shape((BLOCKS, width, width), LOW) for _ in range(packs)]
        + [
            shape((vec.shape[0], width), WIDE),
            shape((count, heads, length), WIDE),
            shape(flat, LOW),
            shape(flat, LOW),
            shape(flat, WIDE),
            shape(flat, LOW),
            shape((BLOCKS,) + flat, WIDE),
            shape((BLOCKS,) + flat, LOW),
            shape((BLOCKS, width, width), LOW),
            shape(qkv, LOW),
            shape(att, LOW),
        ],
        in_specs=[in_vmem] * 7,
        out_specs=[any_space] * packs + [in_vmem] * 2 + [any_space] * 9,
        scratch_shapes=[
            vmem((2, width, width), LOW),
            vmem((n_fsdp,) + vec.shape, LOW),
            vmem(qkv, LOW),
            vmem(qkv, LOW),
            vmem(att, LOW),
            vmem(att, LOW),
            vmem(flat, LOW),
            vmem(flat, LOW),
            vmem(flat, WIDE),
            vmem((2,) + flat, WIDE),
            vmem((2,) + flat, LOW),
            vmem((BLOCKS, depth, width), LOW),
            vmem((2, width, width), LOW),
            *pair(packs, n_z),
            *pair(packs, n_z, 2, BLOCKS - 1),
            *pair(packs, n_z),
            *pair(2 * n_z - 1),
            *pair(count, n_seq),
            *pair(count, n_seq),
            dma((packs + 1,)),
            dma((2,)),
            dma((count,)),
            dma((count,)),
            dma((6,)),
            dma((3, 2)),
        ],
        compiler_params=pltpu.CompilerParams(
            collective_id=0, has_side_effects=True, vmem_limit_bytes=VMEM_LIMIT
        ),
        name="forward_layer",
    )(images, mask, vec, inner_weight, cot, attn, outer)


def add_rows(target, left, right, start, size):
    step = 16 if start % 16 == 0 and size % 16 == 0 else 8

    def body(i, _):
        rows = pl.ds(pl.multiple_of(start + i * step, step), step)
        target[rows, :] = (wide(left[rows, :]) + wide(right[rows, :])).astype(LOW)
        return 0

    lax.fori_loop(0, size // step, body, 0)


class Reduction:
    RING = 4
    Z_RING = 6

    @classmethod
    def scratch(cls, n_seq, n_fsdp, packs, depth, width):
        n_z, upper = n_fsdp // 2, n_seq.bit_length() - 3
        dma, vmem, ring = pltpu.SemaphoreType.DMA, pltpu.VMEM, cls.RING
        piece = (depth, width)
        return [
            vmem((ring, BLOCKS) + piece, LOW),
            vmem((ring, BLOCKS) + piece, LOW),
            vmem((ring, BLOCKS - 1) + piece, LOW),
            vmem((cls.Z_RING,) + piece, LOW),
            vmem((packs, n_z) + piece, LOW),
            vmem((packs, BLOCKS) + piece, LOW),
            vmem((max(upper, 1), ring, BLOCKS) + (piece if upper else (16, 128)), LOW),
            dma((ring,)),
            *pair(ring),
            *pair(ring, 2, BLOCKS - 1),
            *pair(packs, n_z),
            *pair(packs, 2, BLOCKS - 1),
            *pair(max(upper, 1), ring),
            pltpu.SemaphoreType.REGULAR((3 + max(upper, 1),)),
        ]

    def __init__(self, at, packs, grads, scratch):
        self.at, self.packs, self.grads = at, packs, grads
        (
            self.held,
            self.core_in,
            self.plane_in,
            self.z_out,
            self.z_in,
            self.total,
            self.upper_in,
            self.load_sem,
            *sems,
            self.credit,
        ) = scratch
        self.c_sems, self.p_sems, self.z_sems, self.g_sems, self.u_sems = (
            sems[2 * i : 2 * i + 2] for i in range(5)
        )
        self.upper = at.n_seq.bit_length() - 3
        self.count = packs * at.n_z
        self.flight = {}
        self.z_flight = []

    def where(self, i):
        p, t = divmod(i, self.at.n_z)
        return p, t, self.at.across[self.at.n_z - 1 - t], i % self.RING

    def give(self, kind, s, f):
        pl.semaphore_signal(
            self.credit.at[kind], inc=1, device_id={"seq": s, "fsdp": f}, device_id_type=MESH
        )

    def need(self, i, kind):
        if i >= self.RING:
            pl.semaphore_wait(self.credit.at[kind], 1)

    def load(self, i):
        p, _, z, slot = self.where(i)
        rows = self.at.rows(2 * z + self.at.core)
        return pltpu.make_async_copy(
            self.grads[p].at[:, rows], self.held.at[slot], self.load_sem.at[slot]
        )

    def to_partner(self, i):
        p, _, z, slot = self.where(i)
        at = self.at
        rows = at.rows(2 * z + 1 - at.core)
        return at.copy(
            self.grads[p].at[:, rows], self.core_in.at[slot], self.c_sems, slot, at.s, at.other
        )

    def start(self, i):
        if i >= self.RING:
            for copy in self.flight.pop(i - self.RING):
                copy.wait_send()
        self.need(i, 0)
        self.flight[i] = []
        self.go(i, [self.to_partner(i)])
        self.load(i).start()

    def go(self, i, copies):
        for copy in copies:
            copy.start()
            self.flight[i].append(copy)

    def plane(self, i, k):
        at = self.at
        slot = i % self.RING
        for half, steps in enumerate(PLAN):
            bit, masks, first = steps[k]
            for j, m in enumerate(masks):
                src = self.held.at[slot, flip_mask(at.block, m ^ (1 << bit)), at.part(half)]
                dst = self.plane_in.at[slot, first + j, at.part(half)]
                yield at.copy(
                    src, dst, self.p_sems, (slot, half, first + j), flip(at.s, bit), at.f
                )

    def z_copy(self, i, number=0):
        p, t, z, _ = self.where(i)
        at = self.at
        return at.copy(
            self.z_out.at[number % self.Z_RING],
            self.z_in.at[p, t],
            self.z_sems,
            (p, t),
            at.s,
            2 * z + at.core,
        )

    def spread(self, p, k, arriving):
        at = self.at
        for half, steps in enumerate(PLAN):
            bit, masks, slot = steps[k]
            for i, m in enumerate(masks):
                src = self.total.at[p, flip_mask(at.block, m), at.part(half)]
                dst = self.total.at[p, flip_mask(at.block, m ^ (1 << bit)), at.part(half)]
                yield at.copy(
                    src,
                    dst if arriving else src,
                    self.g_sems,
                    (p, half, slot + i),
                    flip(at.s, bit),
                    at.f,
                )

    def add_all(self, slot, term):
        def body(q, _):
            held = self.held.at[slot, q]
            add_rows(held, held, term.at[q], 0, self.at.depth)
            return 0

        lax.fori_loop(0, BLOCKS, body, 0)

    def stage_core(self, i):
        at = self.at
        slot = i % self.RING
        more = i + self.RING < self.count
        self.load(i).wait()
        arrive([self.to_partner(i)])
        self.add_all(slot, self.core_in.at[slot])
        if more:
            self.give(0, at.s, at.other)
        for u in range(self.upper):
            peer = flip(at.s, 2 + u)
            self.need(i, 3 + u)
            copy = at.copy(
                self.held.at[slot], self.upper_in.at[u, slot], self.u_sems, (u, slot), peer, at.f
            )
            copy.start()
            copy.wait()
            self.add_all(slot, self.upper_in.at[u, slot])
            if more:
                self.give(3 + u, peer, at.f)
        self.need(i, 1)
        self.need(i, 2)
        self.go(i, self.plane(i, 1))

    def stage_plane(self, i, k):
        at = self.at
        p, t, _, slot = self.where(i)
        last = t == at.n_z - 1
        arrive(self.plane(i, k))
        number = len(self.z_flight)
        if k == 0 and not last and number >= self.Z_RING:
            self.z_flight[number - self.Z_RING].wait_send()
        for half, steps in enumerate(PLAN):
            _, masks, first = steps[k]
            for j, m in enumerate(masks):
                held = self.held.at[slot, flip_mask(at.block, m)]
                target = held
                if k == 0:
                    target = self.z_in.at[p, t] if last else self.z_out.at[number % self.Z_RING]
                add_rows(target, held, self.plane_in.at[slot, first + j], *at.halves[half])
        if k > 0:
            self.go(i, self.plane(i, k - 1))
            return
        if i + self.RING < self.count:
            for bit in range(2):
                self.give(1 + bit, flip(at.s, bit), at.f)
        if not last:
            copy = self.z_copy(i, number)
            copy.start()
            self.z_flight.append(copy)

    def stage_total(self, p):
        at = self.at
        last = at.n_z - 1
        arrive(self.z_copy(p * at.n_z + t) for t in range(last))

        def body(rows, _):
            value = wide(self.z_in[p, last, rows, :])
            for t in range(last):
                value = value + wide(self.z_in[p, t, rows, :])
            self.total[p, at.block, rows, :] = value.astype(LOW)
            return 0

        row_loop(at.depth, body)
        at.start(self.spread(p, 0, False))

    def stage_spread(self, p, k):
        arrive(self.spread(p, k - 1, True))
        if k < 2:
            self.at.start(self.spread(p, k, False))

    def events(self, i, time):
        return [
            (time, 0, functools.partial(self.stage_core, i)),
            (time + 1, 1, functools.partial(self.stage_plane, i, 1)),
            (time + 2, 2, functools.partial(self.stage_plane, i, 0)),
        ]

    def finish(self):
        for copies in self.flight.values():
            for copy in copies:
                copy.wait_send()
        for copy in self.z_flight[-self.Z_RING :]:
            copy.wait_send()


def backward_kernel(n_seq, n_fsdp, ff_own, *refs):
    refs = list(refs)

    def take(n):
        items = refs[:n]
        del refs[:n]
        return items

    packs = 3
    w_attn, w_inner, w_outer = take(3)
    inner_in, active_in, second_in, hidden_two_in, flat_in, hidden_one_in = take(6)
    images_in, cot_in, grad_outer, qkv_in, attended_in, mask, logsum, vecs = take(8)
    layer_out, images_grad, out_outer, out_attn, inner_grad, vec_out = take(6)
    grads = [grad_outer] + take(packs - 1)
    square, op_one, op_two, act, low, inner, tmp, gs, back = take(9)
    qkv, attended, grad_spread, grad_heads, back_spread, back_in = take(6)
    vec_acc, sums, v_work, v_came, v_z = take(5)
    a_sems, b_sems, v_sems = take(2), take(2), take(2)
    a_local, b_local, s_sem, o_sem, act_sem, g_sem, h_sem, f_sem = take(8)
    rows_all, width = op_one.shape
    count, _, _, group, block = back_in.shape
    heads = group // HD
    depth = width // n_fsdp
    at = Place(n_seq, n_fsdp, depth)
    n_z, bits = at.n_z, n_seq.bit_length() - 1
    red = Reduction(at, packs, grads, refs)
    chunk = lambda p, t: p * n_z + t

    class Load:
        def __init__(self, target, sem):
            self.target, self.sem, self.copy = target, sem, None

        def start(self, src):
            self.copy = pltpu.make_async_copy(src, self.target, self.sem)
            self.copy.start()

        def wait(self):
            self.copy.wait()

    squares = [Load(square.at[k], s_sem.at[k]) for k in range(3)]
    ops = [Load(op_one, o_sem.at[0]), Load(op_two, o_sem.at[1])]
    acts = [Load(act.at[k], act_sem.at[k]) for k in range(2)]
    inners = Load(inner, f_sem.at[0])
    heads_in = [Load(qkv, h_sem.at[0]), Load(attended, h_sem.at[1])]
    stores = {}

    def store(key, src, dst, sem):
        stores[key] = pltpu.make_async_copy(src, dst, sem)
        stores[key].start()

    def stored(*keys):
        for key in keys:
            stores.pop(key).wait()

    send_heads = Exchange(at, grad_spread, grad_heads, a_sems, a_local)
    send_tokens = Exchange(at, back_spread, back_in, b_sems, b_local)

    ops[0].start(cot_in)
    ops[1].start(hidden_two_in)
    squares[2].start(w_outer.at[0])
    squares[0].start(w_inner.at[0])
    inners.start(inner_in.at[0])
    at.greet()

    def mlp(q):
        more = q + 1 < BLOCKS
        if q == 0:
            for copy in ops:
                copy.wait()
        squares[2].wait()
        tmp[...] = product_back(op_one[...], square[2])
        if more:
            squares[2].start(w_outer.at[q + 1])
        else:
            squares[2].start(w_attn.at[3])
        inners.wait()
        sums[0] = jnp.zeros_like(sums[0])

        def body(rows, _):
            value = tmp[rows, :] * gelu_slope(inner[rows, :])
            sums[0] += fold(value)
            low[rows, :] = value.astype(LOW)
            return 0

        row_loop(rows_all, body)
        vec_acc[8 + q : 9 + q, :] = column_sum(sums[0])
        inners.start(inner_in.at[q + 1] if more else second_in)
        squares[0].wait()
        if q == 0:
            gs[...] = product_back(low[...], square[0])
        else:
            gs[...] += product_back(low[...], square[0])
        if more:
            squares[0].start(w_inner.at[q + 1])
        if q > 0:
            stored(("inner", q - 1))
        tall_product(op_two, low, square.at[1])
        store(("inner", q), square.at[1], grads[1].at[q], g_sem.at[1, q])
        if not more:
            ops[1].start(flat_in)

    def second_norm():
        inners.wait()
        for k in range(4):
            sums[k] = jnp.zeros_like(sums[k])

        def body(rows, _):
            normed, factor = normalize(inner[rows, :])
            grad = gs[rows, :]
            up = wide(op_one[rows, :])
            value = up + norm_back(grad * vecs[5:6, :], normed, factor)
            gs[rows, :] = value
            low[rows, :] = value.astype(LOW)
            sums[0] += fold(grad * normed)
            sums[1] += fold(grad)
            sums[2] += fold(value)
            sums[3] += fold(up)
            return 0

        row_loop(rows_all, body)
        for k, row in enumerate((5, 6, 4, 7)):
            vec_acc[row : row + 1, :] = column_sum(sums[k])

    def attended_grad():
        squares[2].wait()
        tmp[...] = product_back(low[...], square[2])
        for i in range(count):
            value = tmp[i * block : (i + 1) * block, :].T.astype(LOW)
            for t in range(n_seq):
                grad_spread[i, t, 0] = value[t * group : (t + 1) * group]
            send_heads.send(i)
        heads_in[0].start(qkv_in.at[0])
        heads_in[1].start(attended_in.at[0])
        stored(("inner", BLOCKS - 1))

    def out_grad():
        ops[1].wait()
        tall_product(op_two, low, square.at[1])
        store(("attn", 3), square.at[1], grads[2].at[3], g_sem.at[2, 3])
        ops[1].start(hidden_one_in)

    def image(i):
        send_heads.receive(i)
        for copy in heads_in:
            copy.wait()
        for w, value in enumerate(
            backward_heads(i, heads, n_seq, qkv, attended, grad_heads.at[i], mask, logsum)
        ):
            scatter_tokens(value, n_seq, back_spread, i, w)
        send_tokens.send(i)
        if i + 1 < count:
            heads_in[0].start(qkv_in.at[i + 1])
            heads_in[1].start(attended_in.at[i + 1])

    def collect(i):
        send_tokens.receive(i)
        for w in range(3):
            features = jnp.concatenate([back_in[i, t, w] for t in range(n_seq)], axis=0)
            back[w, i * block : (i + 1) * block, :] = wide(features).T.astype(LOW)

    def attn_grads():
        ops[1].wait()
        for w in range(3):
            slot = (0, 2, 1)[w]
            if slot == 1:
                stored(("attn", 3))
            tall_product(op_two, back.at[w], square.at[slot])
            store(("attn", w), square.at[slot], grads[2].at[w], g_sem.at[2, w])
        acts[0].start(images_in)
        for w in range(3):
            stored(("attn", w))
            slot = (0, 2, 1)[w]
            squares[slot].start(w_attn.at[w])

    def input_grad():
        for w in range(3):
            slot = (0, 2, 1)[w]
            squares[slot].wait()
            value = product_back(back[w], square[slot])
            if w == 0:
                tmp[...] = value
            else:
                tmp[...] += value
            squares[slot].start(w_outer.at[w])
        acts[0].wait()
        for k in range(4):
            sums[k] = jnp.zeros_like(sums[k])

        def body(rows, _):
            normed, factor = normalize(wide(act[0, rows, :]))
            grad = tmp[rows, :]
            gs[rows, :] += norm_back(grad * vecs[0:1, :], normed, factor)
            sums[0] += fold(grad * normed)
            sums[1] += fold(grad)
            sums[2] += fold(wide(back[0, rows, :]))
            sums[3] += fold(wide(back[2, rows, :]))
            return 0

        row_loop(rows_all, body)
        for k in range(4):
            vec_acc[k : k + 1, :] = column_sum(sums[k])
        store("images", gs, images_grad, f_sem.at[1])
        at.start([vec_copy(0)])
        acts[0].start(active_in.at[0])
        acts[1].start(active_in.at[1])

    def output():
        for q in range(BLOCKS):
            slot = (0, 2, 1, 0)[q]
            squares[slot].wait()
            acts[q % 2].wait()
            inner[...] += product(act[q % 2], square[slot])
            if q == 0:
                squares[0].start(w_outer.at[BLOCKS - 1])
            if q + 2 < BLOCKS:
                acts[q % 2].start(active_in.at[q + 2])

        def body(rows, _):
            inner[rows, :] += vecs[7:8, :]
            return 0

        row_loop(rows_all, body)
        store("layer", inner, layer_out, f_sem.at[2])

    def vec_copy(i):
        src = vec_acc if i == 0 else v_work.at[i - 1]
        peer = (at.s, at.other) if i == 0 else (flip(at.s, i - 1), at.f)
        return at.copy(src, v_came.at[i], v_sems, i, *peer)

    def vec_z(d, arriving):
        z = lax.div(at.from_f[d], 2) if arriving else at.z
        return at.copy(v_work.at[bits], v_z.at[z], v_sems, bits + d, at.s, at.to_f[d])

    def vec_stage(i):
        arrive([vec_copy(i)])
        v_work[i] = (vec_acc[...] if i == 0 else v_work[i - 1]) + v_came[i]
        if i < bits:
            at.start([vec_copy(i + 1)])
        else:
            at.start([vec_z(d, False) for d in range(1, n_z)])

    def vec_last():
        arrive([vec_z(d, True) for d in range(1, n_z)])
        value = v_work[bits]
        for d in range(1, n_z):
            value = value + v_z[lax.div(at.from_f[d], 2)]
        for f in range(n_fsdp):

            @pl.when(at.f == f)
            def _(f=f):
                vec_out[...] = value[:, f * depth : (f + 1) * depth]

    def relayout():
        def body(rows, _):
            parts = []
            for f in range(n_fsdp):
                for q in range(BLOCKS):
                    size = min(depth, ff_own - q * depth)
                    parts.append((q, f * depth, size))
            values = [red.total[1, q, rows, :] for q in range(BLOCKS)]
            inner_grad[rows, :] = jnp.concatenate(
                [values[q][:, first : first + size] for q, first, size in parts], axis=1
            )
            return 0

        row_loop(depth, body)

    def save(p, out):
        store(("out", p), red.total.at[p], out, g_sem.at[p, BLOCKS])

    events = []

    def add(time, call, *args):
        events.append((time, 10, functools.partial(call, *args)))

    gap = 2.5
    first_attn = 2 * n_z + gap
    for i in range(2 * n_z):
        events += red.events(i, i)
        add(-1 if i < red.RING else i - 1.4 if i < n_z else max(i - 1.4, n_z - 0.3), red.start, i)
    for t in range(n_z):
        events += red.events(chunk(2, t), first_attn + t)
        add(first_attn - 0.3 if t < red.RING else first_attn + t - 1.4, red.start, chunk(2, t))
    for q in range(BLOCKS):
        add(q * n_z / BLOCKS * 0.9 + 0.5, mlp, q)
    add(n_z - 0.4, second_norm)
    add(n_z - 0.35, attended_grad)
    add(n_z + 0.5, out_grad)
    for i in range(count):
        add(n_z + 1.5 + i, image, i)
        add(max(n_z + 3.5 + i, first_attn - 1.4 + 0.1 * i), collect, i)
    add(first_attn - 0.4, attn_grads)
    add(first_attn + 0.5, input_grad)
    for i in range(bits + 1):
        add(first_attn + 1.2 + i, vec_stage, i)
    add(first_attn + bits + 2.5, vec_last)
    add(first_attn + 1.5, output)
    for p, last in enumerate((n_z + 1, 2 * n_z + 1, first_attn + n_z + 1)):
        late = 0 if p == packs - 1 else 2
        add(last + late + 1.1, red.stage_total, p)
        add(last + late + 1.8, red.stage_spread, p, 1)
        add(last + late + 2.6, red.stage_spread, p, 2)
    add(n_z + 5.7, save, 0, out_outer)
    add(2 * n_z + 5.7, relayout)
    add(first_attn + n_z + 3.7, save, 2, out_attn)
    run_events(events)
    stored(*list(stores))
    red.finish()
    at.finish()


def run_events(events):
    for _, _, call in sorted(events, key=lambda e: e[:2]):
        call()


def backward_all(n_seq, n_fsdp, ff_own, weights, saved, images, cot, mask, logsum, vecs):
    inner, active, grad_outer, second, hidden_two, flat, hidden_one, qkv, attended = saved
    rows, width = images.shape
    depth, n_z, bits = width // n_fsdp, n_fsdp // 2, n_seq.bit_length() - 1
    count = qkv.shape[0]
    any_space, in_vmem = spaces()
    dma, vmem, shape = pltpu.SemaphoreType.DMA, pltpu.VMEM, jax.ShapeDtypeStruct
    tokens = (rows, width)
    square = (BLOCKS, width, width)
    return pl.pallas_call(
        functools.partial(backward_kernel, n_seq, n_fsdp, ff_own),
        out_shape=[
            shape(tokens, WIDE),
            shape(tokens, WIDE),
            shape((BLOCKS, depth, width), LOW),
            shape((BLOCKS, depth, width), LOW),
            shape((depth, n_fsdp * ff_own), LOW),
            shape((vecs.shape[0], depth), WIDE),
        ]
        + [shape(square, LOW) for _ in range(2)],
        in_specs=[any_space] * 14 + [in_vmem] * 3,
        out_specs=[any_space] * 4 + [in_vmem] * 2 + [any_space] * 2,
        scratch_shapes=[
            vmem((3, width, width), LOW),
            vmem(tokens, LOW),
            vmem(tokens, LOW),
            vmem((2,) + tokens, LOW),
            vmem(tokens, LOW),
            vmem(tokens, WIDE),
            vmem(tokens, WIDE),
            vmem(tokens, WIDE),
            vmem((3,) + tokens, LOW),
            vmem(qkv.shape[1:], LOW),
            vmem(attended.shape[1:], LOW),
            vmem(attended.shape, LOW),
            vmem(attended.shape, LOW),
            vmem(qkv.shape, LOW),
            vmem(qkv.shape, LOW),
            vmem(vecs.shape, WIDE),
            vmem((4, 8, width), WIDE),
            vmem((bits + 1,) + vecs.shape, WIDE),
            vmem((bits + 1,) + vecs.shape, WIDE),
            vmem((n_z,) + vecs.shape, WIDE),
            *pair(count, n_seq),
            *pair(count, n_seq),
            *pair(bits + n_z),
            dma((count,)),
            dma((count,)),
            dma((3,)),
            dma((2,)),
            dma((2,)),
            dma((3, BLOCKS + 1)),
            dma((2,)),
            dma((3,)),
            *Reduction.scratch(n_seq, n_fsdp, 3, depth, width),
        ],
        compiler_params=pltpu.CompilerParams(
            collective_id=1, has_side_effects=True, vmem_limit_bytes=VMEM_LIMIT
        ),
        name="backward_layer",
    )(
        *weights,
        inner,
        active,
        second,
        hidden_two,
        flat,
        hidden_one,
        images,
        cot,
        grad_outer,
        qkv,
        attended,
        mask,
        logsum,
        vecs,
    )


def shards(
    n_seq,
    n_fsdp,
    images,
    key_mask,
    attn_gain,
    attn_shift,
    query_weight,
    key_weight,
    value_weight,
    query_bias,
    value_bias,
    out_weight,
    out_bias,
    mlp_gain,
    mlp_shift,
    inner_weight,
    inner_bias,
    outer_weight,
    outer_bias,
    cotangent,
):
    count, block, width = images.shape
    rows = count * block
    depth = query_weight.shape[0]
    ff_own = outer_weight.shape[0]
    slack = BLOCKS * depth - ff_own
    small = [
        attn_gain,
        attn_shift,
        query_bias,
        value_bias,
        out_bias,
        mlp_gain,
        mlp_shift,
        outer_bias,
    ]
    vec = jnp.concatenate(
        [item.reshape(1, depth) for item in small]
        + [jnp.pad(inner_bias, (0, slack + BLOCKS * depth)).reshape(2 * BLOCKS, depth)]
    )
    mask = jnp.where(key_mask > 0, 0.0, MASKED).astype(WIDE)[:, :, None]
    tokens = images.reshape(rows, width)
    forward = forward_all(
        n_seq,
        n_fsdp,
        count,
        tokens,
        mask,
        vec,
        inner_weight,
        cotangent.reshape(rows, width),
        jnp.stack((query_weight, key_weight, value_weight, out_weight)),
        jnp.pad(outer_weight, ((0, slack), (0, 0))).reshape(BLOCKS, depth, width),
    )
    weights, vecs, logsum = forward[:3], forward[3], forward[4]
    hidden_one, flat, second, hidden_two, inner, active, grad_outer, qkv, attended = forward[5:]
    layer_out, images_grad, outer_sum, attn_sum, inner_grad, vec_sum = backward_all(
        n_seq,
        n_fsdp,
        ff_own,
        weights,
        (inner, active, grad_outer, second, hidden_two, flat, hidden_one, qkv, attended),
        tokens,
        cotangent.reshape(rows, width),
        mask,
        logsum,
        vecs,
    )[:6]
    attn = wide(attn_sum)
    return (
        layer_out.reshape(count, block, width),
        images_grad.reshape(count, block, width),
        vec_sum[0],
        vec_sum[1],
        attn[0],
        attn[1],
        attn[2],
        vec_sum[2],
        vec_sum[3],
        attn[3],
        vec_sum[4],
        vec_sum[5],
        vec_sum[6],
        wide(inner_grad),
        vec_sum[8 : 8 + BLOCKS].reshape(BLOCKS * depth)[:ff_own],
        wide(outer_sum.reshape(BLOCKS * depth, width)[:ff_own]),
        vec_sum[7],
    )


def solution(mesh):
    vector, matrix, tokens = P("fsdp"), P("fsdp", None), P("fsdp", "seq", None)
    params = (
        vector,
        vector,
        matrix,
        matrix,
        matrix,
        vector,
        vector,
        matrix,
        vector,
        vector,
        vector,
        matrix,
        vector,
        matrix,
        vector,
    )
    return jax.shard_map(
        functools.partial(shards, mesh.shape["seq"], mesh.shape["fsdp"]),
        mesh=mesh,
        in_specs=(tokens, matrix) + params + (tokens,),
        out_specs=(tokens, tokens) + params,
        check_vma=False,
    )
```
